256 devices in a mesh: fac: 32 (over y, z), cust: 8 (over x, core).
Axes of the slice: x: 4, y: 4, z: 8, core: 2. Of those that a mesh axis runs over, the one named last changes fastest.
Arguments:
- fac_coords: bfloat16 [16384, 128], P('fac'), may hold values from -6 to 6
- cust_coords: bfloat16 [131072, 128], P(('cust', 'fac')), may hold values from -6 to 6
- open_flags: int32 [16384], P('fac'), may hold values 0 or 1
- demand: int32 [131072], P('cust'), may hold values from 1 to 4
- fixed_cost: float32 [16384], P('fac'), may hold values from 0 to 64
- capacity: float32 [16384], P('fac'), may hold values from 16 to 64
- cap_mult: float32 [16384], P('fac'), may hold values from 0 to 0.1
- cover_mult: float32 [131072], P('cust'), may hold values from 0 to 2, as said below
Outputs:
- cover_final: float32 [131072], P('cust')
- cap_final: float32 [16384], P('fac')
- bounds: float32 [3], replicated
The draws below stay inside these ranges and needn't reach their ends.
Inputs may be any that keep to these rules, and one draw needn't show every extreme that they name: `cover_mult`: initial coverage multipliers, all in one band of width 0.4.
All inputs are finite; a program needn't handle non-finite values. No bound on the sum of `open_flags` on one device may be relied on, other than what follows from the above.
Results may differ from the reference program's by a relative error of at most 0.0003.
Values may be sent and summed in bfloat16 or wider, within the bound.
A program may use at most 64 MiB of HBM per device.

```python
import math
import jax
import jax.numpy as jnp
from jax import lax

K = 128
ITERS = 3
F = 16384
C = 131072


def draw_cover_mult(key, part):
    tau = 0.1
    level = 2.125 - tau * (math.log(F / 2.0) + 300.0 / K)
    spread = jax.random.uniform(key, (C,), jnp.float32, -0.2, 0.2)
    return (level + spread).astype(jnp.float32)


def with_ends(array, rng, smallest, top_value):
    index_at = [jax.random.randint(jax.random.fold_in(rng, axis), (), 0, length) for axis, length in enumerate(array.shape)]
    longest = array.shape.index(max(array.shape))
    neighbour = index_at[:longest] + [(index_at[longest] + 1) % array.shape[longest]] + index_at[longest + 1:]
    return array.at[tuple(index_at)].set(smallest).at[tuple(neighbour)].set(top_value)


def levels(own_key, dims, split, low, high):
    def one(dim, blocks):
        heights = jax.random.uniform(jax.random.fold_in(jax.random.fold_in(own_key, 6), dim), (blocks,), jnp.float32, low / len(split), high / len(split))
        return jnp.repeat(jnp.exp(heights), dims[dim] // blocks).reshape((-1,) + (1,) * (len(dims) - dim - 1))

    loudness = one(*split[0])
    for cut in split[1:]:
        loudness = loudness * one(*cut)
    return loudness


def noise(stream_key, shape, scale, reach, pieces=(), kind=jnp.bfloat16):
    gain = levels(stream_key, shape, pieces, -0.22, 0.18) if pieces else 1.0
    entries = jax.random.normal(stream_key, shape, jnp.float32) * scale * gain
    return jnp.minimum(jnp.maximum(entries, -reach), reach).astype(kind)


def setup_inputs(seed: int = 0) -> dict:
    key_of = jax.random.split(jax.random.key(seed), 9)
    return {
        "fac_coords": noise(key_of[0], (F, K), 1.0, 6.0, ((0, 32),)),
        "cust_coords": noise(key_of[1], (C, K), 1.0, 6.0, ((0, 256),)),
        "open_flags": with_ends((jax.random.randint(key_of[2], (F,), 0, 2) < 1).astype(jnp.int32), jax.random.fold_in(key_of[2], 1), 0, 1),
        "demand": with_ends(jax.random.randint(key_of[3], (C,), 1, 5), jax.random.fold_in(key_of[3], 1), 1, 4).astype(jnp.int32),
        "fixed_cost": jnp.clip(64.0 * jax.random.uniform(key_of[4], (F,), jnp.float32) ** levels(key_of[4], (F,), ((0, 32),), -0.2, 0.2), 0.0, 64.0),
        "capacity": jnp.clip(16.0 + 48.0 * jax.random.uniform(key_of[5], (F,), jnp.float32) ** levels(key_of[5], (F,), ((0, 32),), -0.2, 0.2), 16.0, 64.0),
        "cap_mult": jnp.clip(0.1 * jax.random.uniform(key_of[6], (F,), jnp.float32) ** levels(key_of[6], (F,), ((0, 32),), -0.2, 0.2), 0.0, 0.1),
        "cover_mult": draw_cover_mult(jax.random.fold_in(key_of[8], 71), 0),
    }


def reference(fac_coords, cust_coords, open_flags, demand, fixed_cost, capacity, cap_mult, cover_mult):
    tau = 0.1
    fac_block = 256
    n_fac = fac_coords.shape[0]
    n_cust = cust_coords.shape[0]
    width = fac_coords.shape[1]
    fac_block = min(fac_block, n_fac)
    opened = open_flags.astype(jnp.float32)
    weight = demand.astype(jnp.float32)
    pnorm = jnp.sum(fac_coords.astype(jnp.float32) ** 2, axis=1)
    qnorm = jnp.sum(cust_coords.astype(jnp.float32) ** 2, axis=1)
    blocks = n_fac // fac_block
    lam = cover_mult
    mu = cap_mult
    bound_list = []
    for step in range(ITERS):
        size = 0.1 / (step + 1)

        def one_block(cover, index):
            start = (index * fac_block).astype(jnp.int32)
            rows = lax.dynamic_slice_in_dim(fac_coords, start, fac_block, 0)
            pn = lax.dynamic_slice_in_dim(pnorm, start, fac_block, 0)
            mu_b = lax.dynamic_slice_in_dim(mu, start, fac_block, 0)
            op_b = lax.dynamic_slice_in_dim(opened, start, fac_block, 0)
            dots = lax.dot_general(rows, cust_coords, (((1,), (1,)), ((), ())), preferred_element_type=jnp.float32)
            cost = (pn[:, None] + qnorm[None, :] - 2.0 * dots) / width
            zval = (lam[None, :] - cost - mu_b[:, None] * weight[None, :]) / tau
            share = op_b[:, None] * jax.nn.sigmoid(zval)
            load_b = jnp.sum(share * weight[None, :], axis=1)
            soft_b = -tau * op_b * jnp.sum(jax.nn.softplus(zval) * weight[None, :], axis=1)
            return cover + jnp.sum(share, axis=0), (load_b, soft_b)

        cover, pair = lax.scan(one_block, jnp.zeros((n_cust,), jnp.float32), jnp.arange(blocks, dtype=jnp.int32))
        load = pair[0].reshape(n_fac)
        soft = pair[1].reshape(n_fac)
        bound = (jnp.sum(weight * lam) + jnp.sum(opened * fixed_cost - mu * capacity + soft)) / n_cust
        bound_list.append(bound)
        lam = lam + size * weight * (1.0 - cover) / (1.0 + cover)
        mu = jnp.maximum(0.0, mu + size * (load - capacity) / (load + capacity))
    return lam, mu, jnp.stack(bound_list).astype(jnp.float32)
```

```python
import functools
import math

import jax
import jax.numpy as jnp
from jax import lax
from jax.experimental import pallas as pl
from jax.experimental.pallas import tpu as pltpu
from jax.sharding import PartitionSpec as P

ITERS = 3
CORES = 2
TAU = 0.1
BIG = float(2**20)
LN2 = math.log(2.0)
MESH = pl.DeviceIdType.MESH
F32 = jnp.float32
BF16 = jnp.bfloat16


def split3(v):
    hi = v.astype(BF16).astype(F32)
    rest = v - hi
    mid = rest.astype(BF16).astype(F32)
    lo = (rest - mid).astype(BF16).astype(F32)
    return hi, mid, lo


def place_rows(shape, rows):
    at = lax.broadcasted_iota(jnp.int32, shape, 0)
    out = jnp.zeros(shape, F32)
    for index, row in rows.items():
        out = jnp.where(at == index, jnp.broadcast_to(row, shape), out)
    return out


def fold(v):
    total = v[:, :128]
    for j in range(1, v.shape[1] // 128):
        total = total + v[:, 128 * j : 128 * (j + 1)]
    return total


def kernel(
    ny, nz, nx,
    fac_ref, cust_ref, flag_ref, dem_ref, fix_ref, cap_ref, mu_ref, lam_ref,
    lam_out, mu_out, bound_out,
    fp, fx, r, fv, d8, s0, s1, ld, cv, lg, lam_s, mu_s, pn_s, cap_s, tt,
    cx, l1, l2, fin, tf,
    fp_send, fp_recv, fv_send, fv_recv, r_send, r_recv, fw_send,
    c_send, c_recv, l1_send, l1_recv, l2_send, l2_recv, fin_send, fin_recv, tf_send, tf_recv,
):
    ng = ny * CORES
    half = fac_ref.shape[0] // CORES
    cols = cust_ref.shape[0]
    width = fac_ref.shape[1]
    hrows = half // 128
    crows = cols // 128
    total_cust = float(dem_ref.shape[0] * 128 * nx * CORES)
    f = lax.axis_index("fac")
    c = lax.axis_index("cust")
    y, z = f // nz, f % nz
    x, core = c // CORES, c % CORES
    g = y * CORES + core
    scale = math.log2(math.e) / (width * TAU)

    def at(y_, z_, x_, core_):
        return (y_ * nz + z_, x_ * CORES + core_)

    def z_dev(o):
        zp = (z + o) % nz
        return zp, at(y, zp, x, core)

    def g_dev(o):
        gp = (g + o) % ng
        return gp, at(gp // CORES, z, x, gp % CORES)

    def x_dev(o):
        xp = (x + o) % nx
        return xp, at(y, z, xp, core)

    def near(o, n):
        step = (o + 1) // 2
        return (step * (2 * (o % 2) - 1) + n) % n

    def remote(src, dst, send, recv, dev):
        return pltpu.make_async_remote_copy(
            src_ref=src, dst_ref=dst, send_sem=send, recv_sem=recv, device_id=dev, device_id_type=MESH
        )

    def loop(n, body, start=0):
        lax.fori_loop(start, n, lambda i, _: (body(i), 0)[1], 0)

    barrier = pltpu.get_barrier_semaphore()

    def greet(dev_of, n):
        def body(o):
            pl.semaphore_signal(barrier, inc=1, device_id=dev_of(o)[1], device_id_type=MESH)

        loop(n, body, 1)

    greet(z_dev, nz)
    greet(g_dev, ng)
    greet(x_dev, nx)

    for j in range(crows):
        lanes = slice(128 * j, 128 * (j + 1))
        qt = cust_ref[128 * j : 128 * (j + 1), :].astype(F32).T
        r[g, 0:width, lanes] = (2.0 * qt).astype(BF16)
        qn = jnp.sum(qt * qt, axis=0, keepdims=True)
        dem = dem_ref[pl.ds(f * crows + j, 1), :].astype(F32)
        lam0 = lam_ref[pl.ds(f * crows + j, 1), :]
        qh, qm, ql = split3(-qn)
        one = jnp.ones((1, 128), F32)
        r[g, width : width + 16, lanes] = place_rows(
            (16, 128), {0: qh, 1: qm, 2: ql, 3: -one, 4: -one, 5: -one, 6: -dem, 7: -dem, 8: -dem}
        ).astype(BF16)
        lh, lm, ll = split3(width * lam0)
        r[g, width + 16 : width + 32, lanes] = place_rows((16, 128), {0: lh, 1: lm, 2: ll}).astype(BF16)

    mine = pl.ds(pl.multiple_of(core * half, half), half)
    opened = (flag_ref[pl.ds(core * hrows, hrows), :]).astype(F32)
    for j in range(hrows):
        pt = fac_ref[pl.ds(pl.multiple_of(core * half + 128 * j, 128), 128), :].astype(F32).T
        pn = jnp.sum(pt * pt, axis=0, keepdims=True)
        fv[z, j : j + 1, :] = pn + BIG * (1.0 - opened[j : j + 1])
    fv[z, hrows : 2 * hrows, :] = mu_ref[pl.ds(core * hrows, hrows), :]
    fv[z, 2 * hrows : 3 * hrows, :] = cap_ref[pl.ds(core * hrows, hrows), :]
    fv[z, 3 * hrows : 4 * hrows, :] = jnp.zeros((hrows, 128), F32)
    fp[z] = fac_ref[mine, :]

    pl.semaphore_wait(barrier, (nz - 1) + (ng - 1) + (nx - 1))

    chunk = pl.ds(0, width + 32)

    def fac_copy(o):
        zp, dev = z_dev(near(o, nz))
        return remote(fac_ref.at[mine], fp.at[z], fp_send.at[zp], fp_recv.at[z], dev)

    def vec_copy(o):
        zp, dev = z_dev(near(o, nz))
        return remote(fv.at[z], fv.at[z], fv_send.at[zp], fv_recv.at[z], dev)

    def own_copy(o):
        yp = (y + o) % ny
        return remote(
            r.at[g, chunk], r.at[g, chunk], r_send.at[yp * CORES + core], r_recv.at[g], at(yp, z, x, core)
        )

    def forward(yp):
        s = yp * CORES + core
        return remote(r.at[s, chunk], r.at[s, chunk], fw_send.at[yp], r_recv.at[s], at(y, z, x, 1 - core))

    loop(ny, lambda o: own_copy(o).start(), 1)
    forward(y).start()
    loop(nz, lambda o: vec_copy(o).start(), 1)
    loop(nz, lambda o: fac_copy(o).start(), 1)

    def clear(s):
        r[s, width + 32 :, :] = jnp.zeros((r.shape[1] - width - 32, cols), BF16)

    loop(ng, clear)

    def arrived(o):
        yp = (y + o) % ny
        s = yp * CORES + core
        remote(r.at[s, chunk], r.at[s, chunk], r_send.at[s], r_recv.at[s], at(y, z, x, core)).wait_recv()
        forward(yp).start()

    loop(ny, arrived, 1)

    def from_partner(yp):
        s = yp * CORES + 1 - core
        remote(r.at[s, chunk], r.at[s, chunk], fw_send.at[yp], r_recv.at[s], at(y, z, x, core)).wait_recv()

    loop(ny, from_partner)
    for s in range(ng):
        extra = r[s, width : width + 16, :].astype(F32)
        d8[s] = jnp.broadcast_to(-extra[6:7], (8, cols))
        lam = r[s, width + 16 : width + 32, :].astype(F32)
        lam_s[s : s + 1, :] = (lam[0:1] + lam[1:2] + lam[2:3]) * (1.0 / width)

    def vec_in(o):
        zp = (z + o) % nz
        remote(fv.at[zp], fv.at[zp], fv_send.at[zp], fv_recv.at[zp], at(y, z, x, core)).wait_recv()

    loop(nz, vec_in, 1)
    for zp in range(nz):
        rows = slice(hrows * zp, hrows * (zp + 1))
        pn_s[rows, :] = fv[zp, 0:hrows, :]
        mu_s[rows, :] = fv[zp, hrows : 2 * hrows, :]
        cap_s[rows, :] = fv[zp, 2 * hrows : 3 * hrows, :]

    def build_extra(b):
        for j in range(hrows):
            ph, pm, pll = split3(pn_s[pl.ds(b * hrows + j, 1), :])
            mh, mm, ml = split3(width * mu_s[pl.ds(b * hrows + j, 1), :])
            one = jnp.ones((1, 128), F32)
            top = place_rows(
                (24, 128),
                {0: one, 1: one, 2: one, 3: ph, 4: pm, 5: pll, 6: mh, 7: mm, 8: ml, 16: one, 17: one, 18: one},
            )
            block = jnp.concatenate([top, jnp.zeros((104, 128), F32)], axis=0)
            fx[b, 128 * j : 128 * (j + 1), :] = block.T.astype(BF16)

    loop(nz, build_extra)

    def fac_in(o):
        zp, _ = z_dev(near(o, nz))
        remote(fp.at[zp], fp.at[zp], fp_send.at[zp], fp_recv.at[zp], at(y, z, x, core)).wait_recv()

    loop(nz, fac_in, 1)
    loop(nz, lambda o: fac_copy(o).wait_send(), 1)
    loop(nz, lambda o: vec_copy(o).wait_send(), 1)
    loop(ny, lambda o: own_copy(o).wait_send(), 1)
    loop(ny, lambda yp: forward(yp).wait_send())

    tiles = nz * ng

    def product(slot, t):
        b, s = t // ng, t % ng
        rows = jnp.concatenate([fp[b], fx[b]], axis=1)
        slot[...] = jnp.dot(rows, r[s], preferred_element_type=F32)

    def pointwise(slot, t):
        b, s = t // ng, t % ng
        cov = cv[s]
        logs = lg[s]
        dem = d8[s]
        prod, count = None, 0
        groups = half // 8
        for i in range(groups):
            e = jnp.exp2(slot[8 * i : 8 * i + 8, :] * scale)
            u = 1.0 + e
            share = e / u
            cov = cov + share
            ld[b, 8 * i : 8 * i + 8, :] += fold(share * dem)
            prod = u if prod is None else prod * u
            count += 1
            if count == 3 or i == groups - 1:
                logs = logs + jnp.log2(prod)
                prod, count = None, 0
        cv[s] = cov
        lg[s] = logs

    def step(k):
        size = jnp.where(k == 0, 0.1, jnp.where(k == 1, 0.1 / 2, 0.1 / 3)).astype(F32)

        def zero_rows(b):
            ld[b] = jnp.zeros((half, 128), F32)

        def zero_cols(s):
            cv[s] = jnp.zeros((8, cols), F32)
            lg[s] = jnp.zeros((8, cols), F32)

        loop(nz, zero_rows)
        loop(ng, zero_cols)
        product(s0, 0)

        def two(i):
            t = 2 * i
            product(s1, t + 1)
            pointwise(s0, t)
            product(s0, lax.rem(t + 2, tiles))
            pointwise(s1, t + 1)

        loop(tiles // 2, two)

        def load_row(b):
            for j in range(hrows):
                block = ld[b, 128 * j : 128 * (j + 1), :].T
                l1[k, x, pl.ds(b * hrows + j, 1), :] = jnp.sum(block, axis=0, keepdims=True)

        loop(nz, load_row)
        soft = jnp.zeros((8, cols), F32)
        for s in range(ng):
            soft = soft + lg[s] * d8[s]
        soft = jnp.sum(fold(soft), axis=0, keepdims=True)
        priced = fold(lam_s[pl.ds(g, 1), :] * d8[g][0:1])
        own = pl.ds(z * hrows, hrows)
        rowterm = opened * fix_ref[pl.ds(core * hrows, hrows), :] - mu_s[own, :] * cap_s[own, :]
        rowterm = jnp.sum(rowterm, axis=0, keepdims=True) * (1.0 / nx)
        tt[pl.ds(k, 1), :] = priced + rowterm - (TAU * LN2) * soft
        l1[k, x, hrows * nz :, :] = tt[...]

        def l1_copy(o):
            xp, dev = x_dev(o)
            return remote(l1.at[k, x], l1.at[k, x], l1_send.at[k, xp], l1_recv.at[k, x], dev)

        loop(nx, lambda o: l1_copy(o).start(), 1)
        cx[k, g] = jnp.concatenate([jnp.sum(cv[s], axis=0, keepdims=True) for s in range(ng)], axis=0)

        def c_copy(o):
            gp, dev = g_dev(o)
            return remote(cx.at[k, g], cx.at[k, g], c_send.at[k, gp], c_recv.at[k, g], dev)

        loop(ng, lambda o: c_copy(o).start(), 1)

        def l1_in(o):
            xp, dev = x_dev(o)
            remote(l1.at[k, xp], l1.at[k, xp], l1_send.at[k, xp], l1_recv.at[k, xp], dev).wait_recv()

        loop(nx, l1_in, 1)
        part = l1[k, 0]
        for xp in range(1, nx):
            part = part + l1[k, xp]
        l2[k, z] = part

        def l2_copy(o):
            zp, dev = z_dev(near(o, nz))
            return remote(l2.at[k, z], l2.at[k, z], l2_send.at[k, zp], l2_recv.at[k, z], dev)

        loop(nz, lambda o: l2_copy(o).start(), 1)

        def c_in(o):
            gp, dev = g_dev(o)
            remote(cx.at[k, gp], cx.at[k, gp], c_send.at[k, gp], c_recv.at[k, gp], dev).wait_recv()

        loop(ng, c_in, 1)
        cover = cx[k, 0]
        for gp in range(1, ng):
            cover = cover + cx[k, gp]
        dem = jnp.concatenate([d8[s][0:1] for s in range(ng)], axis=0)
        lam_s[...] = lam_s[...] + size * dem * (1.0 - cover) / (1.0 + cover)
        for s in range(ng):
            lh, lm, ll = split3(width * lam_s[s : s + 1, :])
            r[s, width + 16 : width + 32, :] = place_rows((16, cols), {0: lh, 1: lm, 2: ll}).astype(BF16)

        def l2_in(o):
            zp, dev = z_dev(o)
            remote(l2.at[k, zp], l2.at[k, zp], l2_send.at[k, zp], l2_recv.at[k, zp], dev).wait_recv()

        loop(nz, l2_in, 1)
        whole = l2[k, 0]
        for zp in range(1, nz):
            whole = whole + l2[k, zp]
        load = whole[: hrows * nz]
        tt_all = whole[hrows * nz :]
        cap = cap_s[...]
        mu_s[...] = jnp.maximum(0.0, mu_s[...] + size * (load - cap) / (load + cap))
        loop(nz, build_extra)
        tf[g] = tt_all

        loop(nx, lambda o: l1_copy(o).wait_send(), 1)
        loop(ng, lambda o: c_copy(o).wait_send(), 1)
        loop(nz, lambda o: l2_copy(o).wait_send(), 1)

    tt[...] = jnp.zeros((8, 128), F32)
    loop(ITERS, step)

    for yp in range(ny):
        row = lam_s[pl.ds(yp * CORES + core, 1), :]
        for j in range(crows):
            fin[z, yp * crows + j : yp * crows + j + 1, :] = row[:, 128 * j : 128 * (j + 1)]

    def fin_copy(o):
        zp, dev = z_dev(near(o, nz))
        return remote(fin.at[z], fin.at[z], fin_send.at[zp], fin_recv.at[z], dev)

    loop(nz, lambda o: fin_copy(o).start(), 1)
    own_mu = mu_s[pl.ds(z * hrows, hrows), :]
    tf[g, ITERS : ITERS + hrows, :] = own_mu

    def tf_copy(o):
        gp, dev = g_dev(o)
        return remote(tf.at[g], tf.at[g], tf_send.at[gp], tf_recv.at[g], dev)

    loop(ng, lambda o: tf_copy(o).start(), 1)

    def tf_in(o):
        gp, dev = g_dev(o)
        remote(tf.at[gp], tf.at[gp], tf_send.at[gp], tf_recv.at[gp], dev).wait_recv()

    loop(ng, tf_in, 1)
    total = tf[0]
    for gp in range(1, ng):
        total = total + tf[gp]
    sums = jnp.sum(total, axis=1, keepdims=True) * (1.0 / total_cust)
    bound_out[...] = jnp.broadcast_to(sums, (8, 128))
    for h in range(CORES):
        mu_out[h * hrows : (h + 1) * hrows, :] = tf[y * CORES + h, ITERS : ITERS + hrows, :]

    def fin_in(o):
        zp, dev = z_dev(o)
        remote(fin.at[zp], fin.at[zp], fin_send.at[zp], fin_recv.at[zp], dev).wait_recv()

    loop(nz, fin_in, 1)
    for yp in range(ny):
        for zp in range(nz):
            first = (yp * nz + zp) * crows
            lam_out[first : first + crows, :] = fin[zp, yp * crows : (yp + 1) * crows, :]

    loop(nz, lambda o: fin_copy(o).wait_send(), 1)
    loop(ng, lambda o: tf_copy(o).wait_send(), 1)


def local(dims, fac_coords, cust_coords, open_flags, demand, fixed_cost, capacity, cap_mult, cover_mult):
    ny, nz, nx = dims
    ng = ny * CORES
    fac_n, width = fac_coords.shape
    half = fac_n // CORES
    cols = cust_coords.shape[0]
    hrows = half // 128
    crows = cols // 128
    lrows = hrows * nz + 8
    assert hrows * 4 <= 8 and ITERS + hrows <= 8 and lrows % 8 == 0
    view = lambda a: a.reshape(-1, 128)
    vmem = pl.BlockSpec(memory_space=pltpu.VMEM)
    dma = pltpu.SemaphoreType.DMA
    lam, mu, bounds = pl.pallas_call(
        functools.partial(kernel, ny, nz, nx),
        out_shape=(
            jax.ShapeDtypeStruct((demand.shape[0] // 128, 128), F32),
            jax.ShapeDtypeStruct((fac_n // 128, 128), F32),
            jax.ShapeDtypeStruct((8, 128), F32),
        ),
        in_specs=[vmem] * 8,
        out_specs=(vmem,) * 3,
        scratch_shapes=[
            pltpu.VMEM((nz, half, width), BF16),
            pltpu.VMEM((nz, half, 128), BF16),
            pltpu.VMEM((ng, width + 128, cols), BF16),
            pltpu.VMEM((nz, 8, 128), F32),
            pltpu.VMEM((ng, 8, cols), F32),
            pltpu.VMEM((half, cols), F32),
            pltpu.VMEM((half, cols), F32),
            pltpu.VMEM((nz, half, 128), F32),
            pltpu.VMEM((ng, 8, cols), F32),
            pltpu.VMEM((ng, 8, cols), F32),
            pltpu.VMEM((ng, cols), F32),
            pltpu.VMEM((hrows * nz, 128), F32),
            pltpu.VMEM((hrows * nz, 128), F32),
            pltpu.VMEM((hrows * nz, 128), F32),
            pltpu.VMEM((8, 128), F32),
            pltpu.VMEM((ITERS, ng, ng, cols), F32),
            pltpu.VMEM((ITERS, nx, lrows, 128), F32),
            pltpu.VMEM((ITERS, nz, lrows, 128), F32),
            pltpu.VMEM((nz, ny * crows, 128), F32),
            pltpu.VMEM((ng, 8, 128), F32),
            dma((nz,)), dma((nz,)), dma((nz,)), dma((nz,)), dma((ng,)), dma((ng,)), dma((ny,)),
            dma((ITERS, ng)), dma((ITERS, ng)), dma((ITERS, nx)), dma((ITERS, nx)),
            dma((ITERS, nz)), dma((ITERS, nz)), dma((nz,)), dma((nz,)), dma((ng,)), dma((ng,)),
        ],
        compiler_params=pltpu.CompilerParams(
            collective_id=0, has_side_effects=True, vmem_limit_bytes=48 * 1024 * 1024
        ),
        name="dual",
    )(
        fac_coords, cust_coords, view(open_flags), view(demand), view(fixed_cost), view(capacity),
        view(cap_mult), view(cover_mult),
    )
    return lam.reshape(-1), mu.reshape(-1), bounds[:ITERS, 0]


def solution(mesh, dims=(4, 8, 4)):
    return jax.shard_map(
        functools.partial(local, dims),
        mesh=mesh,
        in_specs=(
            P("fac", None),
            P(("cust", "fac"), None),
            P("fac"),
            P("cust"),
            P("fac"),
            P("fac"),
            P("fac"),
            P("cust"),
        ),
        out_specs=(P("cust"), P("fac"), P()),
        check_vma=False,
    )
```

```python
import functools
import math

import jax
import jax.numpy as jnp
from jax import lax
from jax.experimental import pallas as pl
from jax.experimental.pallas import tpu as pltpu
from jax.sharding import PartitionSpec as P

ITERS = 3
CORES = 2
TAU = 0.1
BIG = float(2**20)
LN2 = math.log(2.0)
MESH = pl.DeviceIdType.MESH
F32 = jnp.float32
BF16 = jnp.bfloat16


def split3(v):
    hi = v.astype(BF16).astype(F32)
    rest = v - hi
    mid = rest.astype(BF16).astype(F32)
    lo = (rest - mid).astype(BF16).astype(F32)
    return hi, mid, lo


def place_rows(shape, rows):
    at = lax.broadcasted_iota(jnp.int32, shape, 0)
    out = jnp.zeros(shape, F32)
    for index, row in rows.items():
        out = jnp.where(at == index, jnp.broadcast_to(row, shape), out)
    return out


def fold(v):
    total = v[:, :128]
    for j in range(1, v.shape[1] // 128):
        total = total + v[:, 128 * j : 128 * (j + 1)]
    return total


def kernel(
    ny, nz, nx, tall,
    fac_hbm, cust_hbm, flag_hbm, dem_hbm, fix_hbm, cap_hbm, mu_hbm, lam_hbm,
    lam_out, mu_out, bound_out,
    fac_ref, cust_ref, flag_ref, dem_ref, fix_ref, cap_ref, mu_ref, lam_ref, in_sem,
    fp, fx, r, fv, d8, s0, s1, ld, cv, lg, lam_s, mu_s, pn_s, cap_s, tt,
    cx, l1, l2, fin, tf,
    fp_send, fp_recv, fv_send, fv_recv, r_send, r_recv, fw_send,
    c_send, c_recv, l1_send, l1_recv, l2_send, l2_recv, fin_send, fin_recv, tf_send, tf_recv,
):
    ng = ny * CORES
    half = fac_ref.shape[0] // CORES
    cols = cust_ref.shape[0]
    width = fac_ref.shape[1]
    hrows = half // 128
    crows = cols // 128
    lrows = hrows * nz
    total_cust = float(dem_ref.shape[0] * 128 * nx * CORES)
    f = lax.axis_index("fac")
    c = lax.axis_index("cust")
    y, z = f // nz, f % nz
    x, core = c // CORES, c % CORES
    g = y * CORES + core
    scale = math.log2(math.e) / (width * TAU)

    pairs = (
        (cust_hbm, cust_ref), (fac_hbm, fac_ref), (flag_hbm, flag_ref), (dem_hbm, dem_ref),
        (lam_hbm, lam_ref), (mu_hbm, mu_ref), (cap_hbm, cap_ref), (fix_hbm, fix_ref),
    )
    loads_in = [pltpu.make_async_copy(a, b, in_sem.at[n]) for n, (a, b) in enumerate(pairs)]
    for copy in loads_in:
        copy.start()

    def at(y_, z_, x_, core_):
        return (y_ * nz + z_, x_ * CORES + core_)

    def near(o, n):
        step = (o + 1) // 2
        return lax.rem(step * (2 * lax.rem(o, 2) - 1) + n, n)

    def z_at(o):
        return lax.rem(z + near(o, nz), nz)

    def y_at(o):
        return lax.rem(y + near(o, ny), ny)

    def z_dev(o):
        zp = z_at(o)
        return zp, at(y, zp, x, core)

    def g_dev(o):
        gp = lax.rem(g + o, ng)
        return gp, at(gp // CORES, z, x, lax.rem(gp, CORES))

    def x_dev(o):
        xp = lax.rem(x + o, nx)
        return xp, at(y, z, xp, core)

    me = at(y, z, x, core)

    def remote(src, dst, send, recv, dev):
        return pltpu.make_async_remote_copy(
            src_ref=src, dst_ref=dst, send_sem=send, recv_sem=recv, device_id=dev, device_id_type=MESH
        )

    def loop(n, body, start=0):
        lax.fori_loop(start, n, lambda i, _: (body(jnp.int32(i)), 0)[1], 0)

    barrier = pltpu.get_barrier_semaphore()

    def greet(dev_of, n):
        def body(o):
            pl.semaphore_signal(barrier, inc=1, device_id=dev_of(o)[1], device_id_type=MESH)

        loop(n, body, 1)

    greet(z_dev, nz)
    greet(g_dev, ng)
    greet(x_dev, nx)

    def zero():
        def zero_rows(b):
            ld[b] = jnp.zeros((half, 128), F32)

        def zero_cols(s):
            cv[s] = jnp.zeros((8, cols), F32)
            lg[s] = jnp.zeros((8, cols), F32)

        loop(nz, zero_rows)
        loop(ng, zero_cols)

    def clear(s):
        r[s, width + 32 :, :] = jnp.zeros((r.shape[1] - width - 32, cols), BF16)

    loop(ng, clear)
    zero()
    tt[...] = jnp.zeros((8, 128), F32)
    for copy in loads_in:
        copy.wait()

    one = jnp.ones((1, 128), F32)
    for j in range(crows):
        lanes = slice(128 * j, 128 * (j + 1))
        qt = cust_ref[128 * j : 128 * (j + 1), :].astype(F32).T
        r[g, 0:width, lanes] = (2.0 * qt).astype(BF16)
        qn = jnp.sum(qt * qt, axis=0, keepdims=True)
        dem = dem_ref[pl.ds(f * crows + j, 1), :].astype(F32)
        lam0 = lam_ref[pl.ds(f * crows + j, 1), :]
        qh, qm, ql = split3(-qn)
        r[g, width : width + 16, lanes] = place_rows(
            (16, 128), {0: qh, 1: qm, 2: ql, 3: -one, 4: -one, 5: -one, 6: -dem, 7: -dem, 8: -dem}
        ).astype(BF16)
        lh, lm, ll = split3(width * lam0)
        r[g, width + 16 : width + 32, lanes] = place_rows((16, 128), {0: lh, 1: lm, 2: ll}).astype(BF16)

    mine = pl.ds(pl.multiple_of(core * half, half), half)
    opened = (flag_ref[pl.ds(core * hrows, hrows), :]).astype(F32)
    for j in range(hrows):
        pt = fac_ref[pl.ds(pl.multiple_of(core * half + 128 * j, 128), 128), :].astype(F32).T
        pn = jnp.sum(pt * pt, axis=0, keepdims=True)
        fv[z, j : j + 1, :] = pn + BIG * (1.0 - opened[j : j + 1])
    fv[z, hrows : 2 * hrows, :] = mu_ref[pl.ds(core * hrows, hrows), :]
    fv[z, 2 * hrows : 3 * hrows, :] = cap_ref[pl.ds(core * hrows, hrows), :]
    fv[z, 3 * hrows : 4 * hrows, :] = jnp.zeros((hrows, 128), F32)
    fp[z] = fac_ref[mine, :]

    pl.semaphore_wait(barrier, (nz - 1) + (ng - 1) + (nx - 1))

    chunk = pl.ds(0, width + 32)

    def fac_copy(o):
        zp, dev = z_dev(o)
        return remote(fac_ref.at[mine], fp.at[z], fp_send.at[zp], fp_recv.at[z], dev)

    def vec_copy(o):
        zp, dev = z_dev(o)
        return remote(fv.at[z], fv.at[z], fv_send.at[zp], fv_recv.at[z], dev)

    def own_copy(o):
        yp = y_at(o)
        return remote(
            r.at[g, chunk], r.at[g, chunk], r_send.at[yp * CORES + core], r_recv.at[g], at(yp, z, x, core)
        )

    def forward(o):
        yp = y_at(o)
        s = yp * CORES + core
        return remote(r.at[s, chunk], r.at[s, chunk], fw_send.at[yp], r_recv.at[s], at(y, z, x, 1 - core))

    loop(nz, lambda o: vec_copy(o).start(), 1)
    loop(ny, lambda o: own_copy(o).start(), 1)
    forward(jnp.int32(0)).start()
    loop(nz, lambda o: fac_copy(o).start(), 1)

    def chunk_at(q):
        return y_at(q // CORES) * CORES + jnp.where(lax.rem(q, CORES) == 0, core, 1 - core)

    def chunk_wait(q):
        s = chunk_at(q)
        remote(r.at[s, chunk], r.at[s, chunk], r_send.at[s], r_recv.at[s], me).wait_recv()

    def chunk_open(q):
        s = chunk_at(q)
        extra = r[s, width : width + 16, :].astype(F32)
        d8[s] = jnp.broadcast_to(-extra[6:7], (8, cols))
        lam = r[s, width + 16 : width + 32, :].astype(F32)
        lam_s[pl.ds(s, 1), :] = (lam[0:1] + lam[1:2] + lam[2:3]) * (1.0 / width)

    def build_extra(b):
        for j in range(hrows):
            ph, pm, pll = split3(pn_s[pl.ds(b * hrows + j, 1), :])
            mh, mm, ml = split3(width * mu_s[pl.ds(b * hrows + j, 1), :])
            top = place_rows(
                (24, 128),
                {0: one, 1: one, 2: one, 3: ph, 4: pm, 5: pll, 6: mh, 7: mm, 8: ml, 16: one, 17: one, 18: one},
            )
            block = jnp.concatenate([top, jnp.zeros((104, 128), F32)], axis=0)
            fx[b, 128 * j : 128 * (j + 1), :] = block.T.astype(BF16)

    def rows_in(first, last):
        for o in range(max(first, 1), last):
            zp = z_at(jnp.int32(o))
            remote(fv.at[zp], fv.at[zp], fv_send.at[zp], fv_recv.at[zp], me).wait_recv()
        for o in range(first, last):
            zp = z_at(jnp.int32(o))
            rows = pl.ds(hrows * zp, hrows)
            pn_s[rows, :] = fv[zp, 0:hrows, :]
            mu_s[rows, :] = fv[zp, hrows : 2 * hrows, :]
            cap_s[rows, :] = fv[zp, 2 * hrows : 3 * hrows, :]
            build_extra(zp)
        for o in range(max(first, 1), last):
            zp = z_at(jnp.int32(o))
            remote(fp.at[zp], fp.at[zp], fp_send.at[zp], fp_recv.at[zp], me).wait_recv()

    tiles = nz * ng // tall
    turns = tiles // 2

    def place(k, t):
        group, q = t // ng, lax.rem(t, ng)
        if k == 0:
            return [z_at(group * tall + j) for j in range(tall)], chunk_at(q)
        return [group * tall + j for j in range(tall)], q

    def product(k, slot, t):
        blocks, s = place(k, t)
        rows = jnp.concatenate(
            [jnp.concatenate([fp[b], fx[b]], axis=1) for b in blocks], axis=0
        )
        slot[...] = jnp.dot(rows, r[s], preferred_element_type=F32)

    def pointwise(k, slot, t):
        blocks, s = place(k, t)
        cov = cv[s]
        logs = lg[s]
        dem = d8[s]
        prod, count = None, 0
        groups = tall * half // 8
        for i in range(groups):
            e = jnp.exp2(slot[8 * i : 8 * i + 8, :] * scale)
            u = 1.0 + e
            share = e / u
            cov = cov + share
            at_row = (8 * i) % half
            ld[blocks[8 * i // half], at_row : at_row + 8, :] += fold(share * dem)
            prod = u if prod is None else prod * u
            count += 1
            if count == 3 or i == groups - 1:
                logs = logs + jnp.log2(prod)
                prod, count = None, 0
        cv[s] = cov
        lg[s] = logs

    parts = (slice(0, lrows // 2), slice(lrows // 2, lrows + 8))

    def load_rows(k, h):
        for b in range(h * nz // 2, (h + 1) * nz // 2):
            for j in range(hrows):
                block = ld[b, 128 * j : 128 * (j + 1), :].T
                at_row = b * hrows + j
                l1[k, x, at_row : at_row + 1, :] = jnp.sum(block, axis=0, keepdims=True)

    def part_ref(ref, k, who, h):
        return ref.at[k, who, pl.ds(parts[h].start, parts[h].stop - parts[h].start)]

    def l1_copy(k, h, o):
        xp, dev = x_dev(o)
        return remote(
            part_ref(l1, k, x, h), part_ref(l1, k, x, h), l1_send.at[2 * k + h, xp], l1_recv.at[2 * k + h, x], dev
        )

    def l2_copy(k, h, o):
        zp, dev = z_dev(o)
        return remote(
            part_ref(l2, k, z, h), part_ref(l2, k, z, h), l2_send.at[2 * k + h, zp], l2_recv.at[2 * k + h, z], dev
        )

    def over_x(k, h):
        def arrived(o):
            xp, dev = x_dev(o)
            part = part_ref(l1, k, xp, h)
            remote(part, part, l1_send.at[2 * k + h, xp], l1_recv.at[2 * k + h, xp], dev).wait_recv()

        loop(nx, arrived, 1)
        part = l1[k, 0, parts[h], :]
        for xp in range(1, nx):
            part = part + l1[k, xp, parts[h], :]
        l2[k, z, parts[h], :] = part
        loop(nz, lambda o: l2_copy(k, h, o).start(), 1)

    def c_copy(k, o):
        gp, dev = g_dev(o)
        return remote(cx.at[k, g], cx.at[k, g], c_send.at[k, gp], c_recv.at[k, g], dev)

    def fin_copy(o):
        zp, dev = z_dev(o)
        return remote(fin.at[z], fin.at[z], fin_send.at[zp], fin_recv.at[z], dev)

    def step(k):
        size = 0.1 / (k + 1)
        last = k == ITERS - 1
        if k == 0:
            rows_in(0, tall)
            chunk_open(jnp.int32(0))
        product(k, s0, jnp.int32(0))

        def two(i):
            t = 2 * i
            if k == 0:

                @pl.when(t + 2 < ng)
                def _():
                    chunk_wait(t + 2)
                    forward((t + 2) // 2).start()
                    chunk_open(t + 2)

                @pl.when(t + 1 < ng)
                def _():
                    chunk_wait(t + 1)
                    chunk_open(t + 1)

                for group in range(1, nz // tall):

                    @pl.when(t + 2 == ng * group)
                    def _():
                        rows_in(group * tall, (group + 1) * tall)

            else:

                @pl.when(i == turns // 2)
                def _():
                    load_rows(k, 0)
                    loop(nx, lambda o: l1_copy(k, 0, o).start(), 1)

                @pl.when(i == turns // 2 + turns // 4)
                def _():
                    over_x(k, 0)

            product(k, s1, t + 1)
            pointwise(k, s0, t)
            product(k, s0, lax.rem(t + 2, tiles))
            pointwise(k, s1, t + 1)

        loop(turns, two)

        if k == 0:
            load_rows(k, 0)
            loop(nx, lambda o: l1_copy(k, 0, o).start(), 1)
        load_rows(k, 1)
        soft = jnp.zeros((8, cols), F32)
        for s in range(ng):
            soft = soft + lg[s] * d8[s]
        soft = jnp.sum(fold(soft), axis=0, keepdims=True)
        priced = fold(lam_s[pl.ds(g, 1), :] * d8[g][0:1])
        own = pl.ds(z * hrows, hrows)
        rowterm = opened * fix_ref[pl.ds(core * hrows, hrows), :] - mu_s[own, :] * cap_s[own, :]
        rowterm = jnp.sum(rowterm, axis=0, keepdims=True) * (1.0 / nx)
        tt[k : k + 1, :] = priced + rowterm - (TAU * LN2) * soft
        l1[k, x, lrows:, :] = tt[...]
        loop(nx, lambda o: l1_copy(k, 1, o).start(), 1)
        cx[k, g] = jnp.concatenate([jnp.sum(cv[s], axis=0, keepdims=True) for s in range(ng)], axis=0)
        loop(ng, lambda o: c_copy(k, o).start(), 1)
        if not last:
            zero()
        if k == 0:
            loop(nz, lambda o: fac_copy(o).wait_send(), 1)
            loop(nz, lambda o: vec_copy(o).wait_send(), 1)
            loop(ny, lambda o: own_copy(o).wait_send(), 1)
            loop(ny, lambda o: forward(o).wait_send())
            over_x(k, 0)
        over_x(k, 1)

        def c_in(o):
            gp, dev = g_dev(o)
            remote(cx.at[k, gp], cx.at[k, gp], c_send.at[k, gp], c_recv.at[k, gp], dev).wait_recv()

        loop(ng, c_in, 1)
        cover = cx[k, 0]
        for gp in range(1, ng):
            cover = cover + cx[k, gp]
        dem = jnp.concatenate([d8[s][0:1] for s in range(ng)], axis=0)
        lam_s[...] = lam_s[...] + size * dem * (1.0 - cover) / (1.0 + cover)
        if last:
            for yp in range(ny):
                row = lam_s[pl.ds(yp * CORES + core, 1), :]
                for j in range(crows):
                    fin[z, yp * crows + j : yp * crows + j + 1, :] = row[:, 128 * j : 128 * (j + 1)]
            loop(nz, lambda o: fin_copy(o).start(), 1)
        else:
            for s in range(ng):
                lh, lm, ll = split3(width * lam_s[s : s + 1, :])
                r[s, width + 16 : width + 32, :] = place_rows((16, cols), {0: lh, 1: lm, 2: ll}).astype(BF16)
        loop(nx, lambda o: l1_copy(k, 0, o).wait_send(), 1)
        loop(nx, lambda o: l1_copy(k, 1, o).wait_send(), 1)
        loop(ng, lambda o: c_copy(k, o).wait_send(), 1)

        def l2_in(o):
            zp, dev = z_dev(o)
            for h in range(2):
                part = part_ref(l2, k, zp, h)
                remote(part, part, l2_send.at[2 * k + h, zp], l2_recv.at[2 * k + h, zp], dev).wait_recv()

        loop(nz, l2_in, 1)
        whole = l2[k, 0]
        for zp in range(1, nz):
            whole = whole + l2[k, zp]
        load = whole[:lrows]
        cap = cap_s[...]
        mu_s[...] = jnp.maximum(0.0, mu_s[...] + size * (load - cap) / (load + cap))
        if last:
            tf[g] = whole[lrows:]
        else:
            for b in range(nz):
                build_extra(b)

    for k in range(ITERS):
        step(k)

    tf[g, ITERS : ITERS + hrows, :] = mu_s[pl.ds(z * hrows, hrows), :]

    def tf_copy(o):
        gp, dev = g_dev(o)
        return remote(tf.at[g], tf.at[g], tf_send.at[gp], tf_recv.at[g], dev)

    loop(ng, lambda o: tf_copy(o).start(), 1)

    def fin_in(o):
        zp, dev = z_dev(o)
        remote(fin.at[zp], fin.at[zp], fin_send.at[zp], fin_recv.at[zp], dev).wait_recv()

    loop(nz, fin_in, 1)
    for yp in range(ny):
        for zp in range(nz):
            first = (yp * nz + zp) * crows
            lam_out[first : first + crows, :] = fin[zp, yp * crows : (yp + 1) * crows, :]
    for k in range(ITERS):
        loop(nz, lambda o: l2_copy(k, 0, o).wait_send(), 1)
        loop(nz, lambda o: l2_copy(k, 1, o).wait_send(), 1)
    loop(nz, lambda o: fin_copy(o).wait_send(), 1)

    def tf_in(o):
        gp, dev = g_dev(o)
        remote(tf.at[gp], tf.at[gp], tf_send.at[gp], tf_recv.at[gp], dev).wait_recv()

    loop(ng, tf_in, 1)
    total = tf[0]
    for gp in range(1, ng):
        total = total + tf[gp]
    sums = jnp.sum(total, axis=1, keepdims=True) * (1.0 / total_cust)
    bound_out[...] = jnp.broadcast_to(sums, (8, 128))
    for h in range(CORES):
        mu_out[h * hrows : (h + 1) * hrows, :] = tf[y * CORES + h, ITERS : ITERS + hrows, :]
    loop(ng, lambda o: tf_copy(o).wait_send(), 1)


def local(dims, fac_coords, cust_coords, open_flags, demand, fixed_cost, capacity, cap_mult, cover_mult):
    ny, nz, nx = dims
    ng = ny * CORES
    fac_n, width = fac_coords.shape
    half = fac_n // CORES
    cols = cust_coords.shape[0]
    hrows = half // 128
    crows = cols // 128
    lrows = hrows * nz + 8
    assert hrows * 4 <= 8 and ITERS + hrows <= 8 and lrows % 8 == 0
    view = lambda a: a.reshape(-1, 128)
    vmem = pl.BlockSpec(memory_space=pltpu.VMEM)
    hbm = pl.BlockSpec(memory_space=pltpu.HBM)
    tall = 4
    dma = pltpu.SemaphoreType.DMA
    lam, mu, bounds = pl.pallas_call(
        functools.partial(kernel, ny, nz, nx, tall),
        out_shape=(
            jax.ShapeDtypeStruct((demand.shape[0] // 128, 128), F32),
            jax.ShapeDtypeStruct((fac_n // 128, 128), F32),
            jax.ShapeDtypeStruct((8, 128), F32),
        ),
        in_specs=[hbm] * 8,
        out_specs=(vmem,) * 3,
        scratch_shapes=[
            pltpu.VMEM((fac_n, width), BF16),
            pltpu.VMEM((cols, width), BF16),
            pltpu.VMEM((fac_n // 128, 128), jnp.int32),
            pltpu.VMEM((demand.shape[0] // 128, 128), jnp.int32),
            pltpu.VMEM((fac_n // 128, 128), F32),
            pltpu.VMEM((fac_n // 128, 128), F32),
            pltpu.VMEM((fac_n // 128, 128), F32),
            pltpu.VMEM((demand.shape[0] // 128, 128), F32),
            dma((8,)),
            pltpu.VMEM((nz, half, width), BF16),
            pltpu.VMEM((nz, half, 128), BF16),
            pltpu.VMEM((ng, width + 128, cols), BF16),
            pltpu.VMEM((nz, 8, 128), F32),
            pltpu.VMEM((ng, 8, cols), F32),
            pltpu.VMEM((tall * half, cols), F32),
            pltpu.VMEM((tall * half, cols), F32),
            pltpu.VMEM((nz, half, 128), F32),
            pltpu.VMEM((ng, 8, cols), F32),
            pltpu.VMEM((ng, 8, cols), F32),
            pltpu.VMEM((ng, cols), F32),
            pltpu.VMEM((hrows * nz, 128), F32),
            pltpu.VMEM((hrows * nz, 128), F32),
            pltpu.VMEM((hrows * nz, 128), F32),
            pltpu.VMEM((8, 128), F32),
            pltpu.VMEM((ITERS, ng, ng, cols), F32),
            pltpu.VMEM((ITERS, nx, lrows, 128), F32),
            pltpu.VMEM((ITERS, nz, lrows, 128), F32),
            pltpu.VMEM((nz, ny * crows, 128), F32),
            pltpu.VMEM((ng, 8, 128), F32),
            dma((nz,)), dma((nz,)), dma((nz,)), dma((nz,)), dma((ng,)), dma((ng,)), dma((ny,)),
            dma((ITERS, ng)), dma((ITERS, ng)), dma((2 * ITERS, nx)), dma((2 * ITERS, nx)),
            dma((2 * ITERS, nz)), dma((2 * ITERS, nz)), dma((nz,)), dma((nz,)), dma((ng,)), dma((ng,)),
        ],
        compiler_params=pltpu.CompilerParams(
            collective_id=0,
            has_side_effects=True,
            vmem_limit_bytes=60 * 1024 * 1024,
        ),
        name="dual",
    )(
        fac_coords, cust_coords, view(open_flags), view(demand), view(fixed_cost), view(capacity),
        view(cap_mult), view(cover_mult),
    )
    return lam.reshape(-1), mu.reshape(-1), bounds[:ITERS, 0]


def solution(mesh, dims=(4, 8, 4)):
    return jax.shard_map(
        functools.partial(local, dims),
        mesh=mesh,
        in_specs=(
            P("fac", None),
            P(("cust", "fac"), None),
            P("fac"),
            P("cust"),
            P("fac"),
            P("fac"),
            P("fac"),
            P("cust"),
        ),
        out_specs=(P("cust"), P("fac"), P()),
        check_vma=False,
    )
```

```python
import functools
import math

import jax
import jax.numpy as jnp
from jax import lax
from jax.experimental import pallas as pl
from jax.experimental.pallas import tpu as pltpu
from jax.sharding import PartitionSpec as P

ITERS = 3
CORES = 2
TAU = 0.1
BIG = float(2**20)
LN2 = math.log(2.0)
MESH = pl.DeviceIdType.MESH
F32 = jnp.float32
BF16 = jnp.bfloat16


def split3(v):
    hi = v.astype(BF16).astype(F32)
    rest = v - hi
    mid = rest.astype(BF16).astype(F32)
    lo = (rest - mid).astype(BF16).astype(F32)
    return hi, mid, lo


def place_rows(shape, rows):
    at = lax.broadcasted_iota(jnp.int32, shape, 0)
    out = jnp.zeros(shape, F32)
    for index, row in rows.items():
        out = jnp.where(at == index, jnp.broadcast_to(row, shape), out)
    return out


def fold(v):
    total = v[:, :128]
    for j in range(1, v.shape[1] // 128):
        total = total + v[:, 128 * j : 128 * (j + 1)]
    return total


def kernel(
    ny, nz, nx, tall,
    fac_hbm, cust_hbm, flag_hbm, dem_hbm, fix_hbm, cap_hbm, mu_hbm, lam_hbm,
    lam_out, mu_out, bound_out,
    fac_ref, cust_ref, flag_ref, dem_ref, fix_ref, cap_ref, mu_ref, lam_ref, in_sem,
    fp, fx, r, fv, d8, dm, s0, s1, ld, cv, soft, lg, lam_s, mu_s, pn_s, cap_s, tt,
    cx, l1, l2, fin, tf,
    fp_send, fp_recv, fv_send, fv_recv, r_send, r_recv, fw_send,
    c_send, c_recv, l1_send, l1_recv, l2_send, l2_recv, fin_send, fin_recv, tf_send, tf_recv,
):
    ng = ny * CORES
    half = fac_ref.shape[0] // CORES
    cols = cust_ref.shape[0]
    width = fac_ref.shape[1]
    hrows = half // 128
    crows = cols // 128
    groups = nz // tall
    grows = tall * hrows
    total_cust = float(dem_ref.shape[0] * 128 * nx * CORES)
    f = lax.axis_index("fac")
    c = lax.axis_index("cust")
    y, z = f // nz, f % nz
    x, core = c // CORES, c % CORES
    g = y * CORES + core
    scale = math.log2(math.e) / (width * TAU)

    pairs = (
        (cust_hbm, cust_ref), (fac_hbm, fac_ref), (flag_hbm, flag_ref), (dem_hbm, dem_ref),
        (lam_hbm, lam_ref), (mu_hbm, mu_ref), (cap_hbm, cap_ref), (fix_hbm, fix_ref),
    )
    loads_in = [pltpu.make_async_copy(a, b, in_sem.at[n]) for n, (a, b) in enumerate(pairs)]
    for copy in loads_in:
        copy.start()

    def at(y_, z_, x_, core_):
        return (y_ * nz + z_, x_ * CORES + core_)

    def near(o, n):
        step = (o + 1) // 2
        return lax.rem(step * (2 * lax.rem(o, 2) - 1) + n, n)

    def z_at(o):
        return lax.rem(z + near(o, nz), nz)

    def y_at(o):
        return lax.rem(y + near(o, ny), ny)

    def z_dev(o):
        zp = z_at(o)
        return zp, at(y, zp, x, core)

    def g_dev(o):
        gp = lax.rem(g + o, ng)
        return gp, at(gp // CORES, z, x, lax.rem(gp, CORES))

    def z_plain(o):
        zp = lax.rem(z + o, nz)
        return zp, at(y, zp, x, core)

    def x_dev(o):
        xp = lax.rem(x + o, nx)
        return xp, at(y, z, xp, core)

    me = at(y, z, x, core)

    def remote(src, dst, send, recv, dev):
        return pltpu.make_async_remote_copy(
            src_ref=src, dst_ref=dst, send_sem=send, recv_sem=recv, device_id=dev, device_id_type=MESH
        )

    def loop(n, body, start=0):
        lax.fori_loop(start, n, lambda i, _: (body(jnp.int32(i)), 0)[1], 0)

    barrier = pltpu.get_barrier_semaphore()

    def greet(dev_of, n):
        def body(o):
            pl.semaphore_signal(barrier, inc=1, device_id=dev_of(o)[1], device_id_type=MESH)

        loop(n, body, 1)

    greet(z_dev, nz)
    greet(g_dev, ng)
    greet(x_dev, nx)

    def zero():
        def zero_rows(b):
            ld[b] = jnp.zeros((half, 128), F32)

        def zero_cols(s):
            cv[s] = jnp.zeros((8, cols), F32)
            lg[s] = jnp.zeros((8, cols), F32)

        loop(nz, zero_rows)
        loop(ng, zero_cols)

    def clear(s):
        r[s, width + 32 :, :] = jnp.zeros((r.shape[1] - width - 32, cols), BF16)

    loop(ng, clear)
    zero()
    tt[...] = jnp.zeros((8, 128), F32)
    soft[...] = jnp.zeros((8, 128), F32)
    for copy in loads_in:
        copy.wait()

    one = jnp.ones((1, 128), F32)
    for j in range(crows):
        lanes = slice(128 * j, 128 * (j + 1))
        qt = cust_ref[128 * j : 128 * (j + 1), :].astype(F32).T
        r[g, 0:width, lanes] = (2.0 * qt).astype(BF16)
        qn = jnp.sum(qt * qt, axis=0, keepdims=True)
        dem = dem_ref[pl.ds(f * crows + j, 1), :].astype(F32)
        lam0 = lam_ref[pl.ds(f * crows + j, 1), :]
        qh, qm, ql = split3(-qn)
        r[g, width : width + 16, lanes] = place_rows(
            (16, 128), {0: qh, 1: qm, 2: ql, 3: -one, 4: -one, 5: -one, 6: -dem, 7: -dem, 8: -dem}
        ).astype(BF16)
        lh, lm, ll = split3(width * lam0)
        r[g, width + 16 : width + 32, lanes] = place_rows((16, 128), {0: lh, 1: lm, 2: ll}).astype(BF16)

    mine = pl.ds(pl.multiple_of(core * half, half), half)
    opened = (flag_ref[pl.ds(core * hrows, hrows), :]).astype(F32)
    for j in range(hrows):
        pt = fac_ref[pl.ds(pl.multiple_of(core * half + 128 * j, 128), 128), :].astype(F32).T
        pn = jnp.sum(pt * pt, axis=0, keepdims=True)
        fv[z, j : j + 1, :] = pn + BIG * (1.0 - opened[j : j + 1])
    fv[z, hrows : 2 * hrows, :] = mu_ref[pl.ds(core * hrows, hrows), :]
    fv[z, 2 * hrows : 3 * hrows, :] = cap_ref[pl.ds(core * hrows, hrows), :]
    fv[z, 3 * hrows : 4 * hrows, :] = jnp.zeros((hrows, 128), F32)
    fp[z] = fac_ref[mine, :]

    pl.semaphore_wait(barrier, (nz - 1) + (ng - 1) + (nx - 1))

    chunk = pl.ds(0, width + 32)

    def fac_copy(o):
        zp, dev = z_dev(o)
        return remote(fac_ref.at[mine], fp.at[z], fp_send.at[zp], fp_recv.at[z], dev)

    def vec_copy(o):
        zp, dev = z_dev(o)
        return remote(fv.at[z], fv.at[z], fv_send, fv_recv, dev)

    def own_copy(o):
        yp = y_at(o)
        return remote(
            r.at[g, chunk], r.at[g, chunk], r_send.at[yp * CORES + core], r_recv.at[g], at(yp, z, x, core)
        )

    def forward(o):
        yp = y_at(o)
        s = yp * CORES + core
        return remote(r.at[s, chunk], r.at[s, chunk], fw_send.at[yp], r_recv.at[s], at(y, z, x, 1 - core))

    loop(nz, lambda o: vec_copy(o).start(), 1)
    loop(ny, lambda o: own_copy(o).start(), 1)
    forward(jnp.int32(0)).start()
    early = z < nz // 2

    @pl.when(early)
    def _():
        loop(nz, lambda o: fac_copy(o).start(), 1)


    def chunk_at(q):
        return y_at(q // CORES) * CORES + jnp.where(lax.rem(q, CORES) == 0, core, 1 - core)

    def chunk_wait(q):
        s = chunk_at(q)
        remote(r.at[s, chunk], r.at[s, chunk], r_send.at[s], r_recv.at[s], me).wait_recv()

    def chunk_open(q):
        s = chunk_at(q)
        extra = r[s, width : width + 16, :].astype(F32)
        dem = -extra[6:7]
        d8[s] = jnp.broadcast_to(dem, (8, cols))
        lam = r[s, width + 16 : width + 32, :].astype(F32)
        lam = (lam[0:1] + lam[1:2] + lam[2:3]) * (1.0 / width)
        first = lax.rem(s, CORES) * crows
        for j in range(crows):
            dm[s // CORES, pl.ds(first + j, 1), :] = dem[:, 128 * j : 128 * (j + 1)]
            lam_s[s // CORES, pl.ds(first + j, 1), :] = lam[:, 128 * j : 128 * (j + 1)]

    def build_extra(b):
        for j in range(hrows):
            ph, pm, pll = split3(pn_s[pl.ds(b * hrows + j, 1), :])
            mh, mm, ml = split3(width * mu_s[pl.ds(b * hrows + j, 1), :])
            top = place_rows(
                (24, 128),
                {0: one, 1: one, 2: one, 3: ph, 4: pm, 5: pll, 6: mh, 7: mm, 8: ml, 16: one, 17: one, 18: one},
            )
            block = jnp.concatenate([top, jnp.zeros((104, 128), F32)], axis=0)
            fx[b, 128 * j : 128 * (j + 1), :] = block.T.astype(BF16)

    def vectors_in():
        others = fv.at[pl.ds(0, nz - 1)]
        remote(others, others, fv_send, fv_recv, me).wait_recv()
        for zp in range(nz):
            rows = slice(hrows * zp, hrows * (zp + 1))
            pn_s[rows, :] = fv[zp, 0:hrows, :]
            mu_s[rows, :] = fv[zp, hrows : 2 * hrows, :]
            cap_s[rows, :] = fv[zp, 2 * hrows : 3 * hrows, :]
        for zp in range(nz):
            build_extra(zp)

    def rows_in(group):
        for zp in range(group * tall, (group + 1) * tall):

            @pl.when(z != zp)
            def _():
                remote(fp.at[zp], fp.at[zp], fp_send.at[zp], fp_recv.at[zp], me).wait_recv()

    tiles = nz * ng // tall
    turns = tiles // 2

    def place(k, t):
        group, q = lax.rem(t // ng, groups), lax.rem(t, ng)
        s = jnp.where(t < ng, chunk_at(q), q) if k == 0 else q
        return [group * tall + j for j in range(tall)], s

    def product(k, slot, t):
        blocks, s = place(k, t)
        rows = jnp.concatenate(
            [jnp.concatenate([fp[b], fx[b]], axis=1) for b in blocks], axis=0
        )
        slot[...] = jnp.dot(rows, r[s], preferred_element_type=F32)

    def pointwise(k, slot, t):
        blocks, s = place(k, t)
        cov = cv[s]
        logs = lg[s]
        dem = d8[s]
        prod, count = None, 0
        parts = tall * half // 8
        for i in range(parts):
            e = jnp.exp2(slot[8 * i : 8 * i + 8, :] * scale)
            u = 1.0 + e
            share = e / u
            cov = cov + share
            at_row = (8 * i) % half
            ld[blocks[8 * i // half], at_row : at_row + 8, :] += fold(share * dem)
            prod = u if prod is None else prod * u
            count += 1
            if count == 3 or i == parts - 1:
                logs = logs + jnp.log2(prod)
                prod, count = None, 0
        cv[s] = cov
        lg[s] = logs

    def l1_copy(n, o):
        xp, dev = x_dev(o)
        return remote(l1.at[n, x], l1.at[n, x], l1_send.at[n], l1_recv.at[n], dev)

    def l2_copy(n, o):
        zp, dev = z_plain(o)
        return remote(l2.at[n, z], l2.at[n, z], l2_send.at[n], l2_recv.at[n], dev)

    def c_copy(n, o):
        gp, dev = g_dev(o)
        return remote(cx.at[n, g], cx.at[n, g], c_send.at[n], c_recv.at[n], dev)

    def fin_copy(o):
        zp, dev = z_plain(o)
        return remote(fin.at[z], fin.at[z], fin_send, fin_recv, dev)

    def all_of(ref, n, count, send, recv):
        others = ref.at[n, pl.ds(0, count - 1)]
        return remote(others, others, send.at[n], recv.at[n], me)

    def loads_out(k, group):
        n = k * groups + group
        rows = []
        for b in range(group * tall, (group + 1) * tall):
            for j in range(hrows):
                block = ld[b, 128 * j : 128 * (j + 1), :].T
                rows.append(jnp.sum(block, axis=0, keepdims=True))
        l1[n, x] = jnp.concatenate(rows + [tt[0 : 8 - grows, :]], axis=0)
        loop(nx, lambda o: l1_copy(n, o).start(), 1)
        for b in range(group * tall, (group + 1) * tall):
            ld[b] = jnp.zeros((half, 128), F32)

    def loads_on(k, group):
        n = k * groups + group
        all_of(l1, n, nx, l1_send, l1_recv).wait_recv()
        part = l1[n, 0]
        for xp in range(1, nx):
            part = part + l1[n, xp]
        l2[n, z] = part
        loop(nz, lambda o: l2_copy(n, o).start(), 1)

    def loads_in_use(k, group):
        n = k * groups + group
        all_of(l2, n, nz, l2_send, l2_recv).wait_recv()
        whole = l2[n, 0]
        for zp in range(1, nz):
            whole = whole + l2[n, zp]
        load = whole[:grows]
        rows = slice(group * grows, (group + 1) * grows)
        cap = cap_s[rows, :]
        size = 0.1 / (k + 1)
        mu_s[rows, :] = jnp.maximum(0.0, mu_s[rows, :] + size * (load - cap) / (load + cap))
        if k < ITERS - 1:
            for b in range(group * tall, (group + 1) * tall):
                build_extra(b)
        elif group == groups - 1:
            tf[g] = jnp.concatenate([whole[grows:], jnp.zeros((grows, 128), F32)], axis=0)

    def cover_out(k, pair):
        n = k * ny + pair
        rows = []
        for s in range(pair * CORES, (pair + 1) * CORES):
            cov = jnp.sum(cv[s], axis=0, keepdims=True)
            rows += [cov[:, 128 * j : 128 * (j + 1)] for j in range(crows)]
        cx[n, g] = jnp.concatenate(rows, axis=0)
        loop(ng, lambda o: c_copy(n, o).start(), 1)
        total = soft[...]
        for s in range(pair * CORES, (pair + 1) * CORES):
            total = total + fold(lg[s] * d8[s])
            cv[s] = jnp.zeros((8, cols), F32)
            lg[s] = jnp.zeros((8, cols), F32)
        soft[...] = total
        if pair == ny - 1:
            tt[k : k + 1, :] = tt[k : k + 1, :] - (TAU * LN2) * jnp.sum(total, axis=0, keepdims=True)
            soft[...] = jnp.zeros((8, 128), F32)

    def cover_in_use(k, pair):
        n = k * ny + pair
        all_of(cx, n, ng, c_send, c_recv).wait_recv()
        cover = cx[n, 0]
        for gp in range(1, ng):
            cover = cover + cx[n, gp]
        size = 0.1 / (k + 1)
        lam = lam_s[pair] + size * dm[pair] * (1.0 - cover) / (1.0 + cover)
        lam_s[pair] = lam
        if k < ITERS - 1:
            lh, lm, ll = split3(width * lam)
            for m in range(CORES * crows):
                s, j = pair * CORES + m // crows, m % crows
                r[s, width + 16 : width + 32, 128 * j : 128 * (j + 1)] = place_rows(
                    (16, 128), {0: lh[m : m + 1], 1: lm[m : m + 1], 2: ll[m : m + 1]}
                ).astype(BF16)

    def terms(k):
        mine_rows = pl.ds(core * crows, crows)
        priced = jnp.sum(lam_s[y, mine_rows, :] * dm[y, mine_rows, :], axis=0, keepdims=True)
        own = pl.ds(z * hrows, hrows)
        rowterm = opened * fix_ref[pl.ds(core * hrows, hrows), :] - mu_s[own, :] * cap_s[own, :]
        tt[k : k + 1, :] = priced + jnp.sum(rowterm, axis=0, keepdims=True) * (1.0 / nx)

    span = ng // 2

    def events(k, i):
        def when(turn, *jobs):
            @pl.when(i == turn)
            def _():
                for job in jobs:
                    job()

        job = functools.partial
        last = groups - 1
        table = {}

        def add(turn, *args):
            table.setdefault(turn, []).append(job(*args))

        if k:
            add(0, cover_out, k - 1, ny - 1)
            add(0, loads_out, k - 1, last)
        for pair in range(ny - 1):
            add(span * last + 1 + pair, cover_out, k, pair)
        for group in range(last):
            add(span * (group + 1), loads_out, k, group)
        if k == 0:
            def sent():
                loop(nz, lambda o: fac_copy(o).wait_send(), 1)
                loop(ny, lambda o: own_copy(o).wait_send(), 1)
                loop(ny, lambda o: forward(o).wait_send())

            add(turns - 2, sent)
            for group in range(1, groups):
                add(span * group - 1, rows_in, group)
        else:
            for pair in range(1, ny):
                add(pair - 1, cover_in_use, k - 1, pair)
            add(span - 1, loads_on, k - 1, last)
        add(span * last - 1, terms, k)
        for group in range(last):
            add(span * (group + 1) + span - 1, loads_on, k, group)
        for group in range(groups):
            turn = span * (group + 3)
            if turn < turns:
                add(turn, loads_in_use, k, group)
            elif k < ITERS - 1:
                pass
        if k:
            for group in range(groups):
                turn = span * (group + 3)
                if turn >= turns:
                    add(turn - turns, loads_in_use, k - 1, group)
        if k < ITERS - 1:
            add(turns - 1, cover_in_use, k, 0)
        for turn in sorted(table):
            when(turn, *table[turn])

    def step(k):
        def two(i):
            t = 2 * i
            if k == 0:

                @pl.when(t + 2 < ng)
                def _():
                    chunk_wait(t + 2)
                    forward((t + 2) // 2).start()
                    chunk_open(t + 2)

                @pl.when(t + 1 < ng)
                def _():
                    chunk_wait(t + 1)
                    chunk_open(t + 1)

            events(k, i)
            product(k, s1, t + 1)
            pointwise(k, s0, t)
            product(k, s0, t + 2)
            pointwise(k, s1, t + 1)

        loop(turns, two)

    chunk_open(jnp.int32(0))
    vectors_in()

    @pl.when(jnp.logical_not(early))
    def _():
        loop(nz, lambda o: fac_copy(o).start(), 1)

    rows_in(0)
    product(0, s0, jnp.int32(0))
    for k in range(ITERS):
        step(k)

    k, last = ITERS - 1, groups - 1
    cover_out(k, ny - 1)
    loads_out(k, last)
    for group in range(groups):
        if span * (group + 3) >= turns and group < last:
            loads_in_use(k, group)
    loads_on(k, last)
    for pair in range(ny):
        cover_in_use(k, pair)
    for yp in range(ny):
        fin[z, yp * crows : (yp + 1) * crows, :] = lam_s[yp, pl.ds(core * crows, crows), :]
    loop(nz, lambda o: fin_copy(o).start(), 1)
    for n in range(ITERS * groups):
        all_of(l1, n, nx, l1_send, l1_recv).wait_send()
    for n in range(ITERS * ny):
        all_of(cx, n, ng, c_send, c_recv).wait_send()
    remote(fv.at[pl.ds(0, nz - 1)], fv.at[pl.ds(0, nz - 1)], fv_send, fv_recv, me).wait_send()
    loads_in_use(k, last)

    tf[g, ITERS : ITERS + hrows, :] = mu_s[pl.ds(z * hrows, hrows), :]

    def tf_copy(o):
        gp, dev = g_dev(o)
        return remote(tf.at[g], tf.at[g], tf_send, tf_recv, dev)

    loop(ng, lambda o: tf_copy(o).start(), 1)

    others = fin.at[pl.ds(0, nz - 1)]
    remote(others, others, fin_send, fin_recv, me).wait_recv()
    for yp in range(ny):
        for zp in range(nz):
            first = (yp * nz + zp) * crows
            lam_out[first : first + crows, :] = fin[zp, yp * crows : (yp + 1) * crows, :]
    for n in range(ITERS * groups):
        all_of(l2, n, nz, l2_send, l2_recv).wait_send()
    remote(others, others, fin_send, fin_recv, me).wait_send()
    peers = tf.at[pl.ds(0, ng - 1)]
    remote(peers, peers, tf_send, tf_recv, me).wait_recv()
    total = tf[0]
    for gp in range(1, ng):
        total = total + tf[gp]
    sums = jnp.sum(total, axis=1, keepdims=True) * (1.0 / total_cust)
    bound_out[...] = jnp.broadcast_to(sums, (8, 128))
    for h in range(CORES):
        mu_out[h * hrows : (h + 1) * hrows, :] = tf[y * CORES + h, ITERS : ITERS + hrows, :]
    remote(peers, peers, tf_send, tf_recv, me).wait_send()


def local(dims, fac_coords, cust_coords, open_flags, demand, fixed_cost, capacity, cap_mult, cover_mult):
    ny, nz, nx = dims
    ng = ny * CORES
    fac_n, width = fac_coords.shape
    half = fac_n // CORES
    cols = cust_coords.shape[0]
    hrows = half // 128
    crows = cols // 128
    view = lambda a: a.reshape(-1, 128)
    vmem = pl.BlockSpec(memory_space=pltpu.VMEM)
    hbm = pl.BlockSpec(memory_space=pltpu.HBM)
    tall = 2
    groups = nz // tall
    dma = pltpu.SemaphoreType.DMA
    lam, mu, bounds = pl.pallas_call(
        functools.partial(kernel, ny, nz, nx, tall),
        out_shape=(
            jax.ShapeDtypeStruct((demand.shape[0] // 128, 128), F32),
            jax.ShapeDtypeStruct((fac_n // 128, 128), F32),
            jax.ShapeDtypeStruct((8, 128), F32),
        ),
        in_specs=[hbm] * 8,
        out_specs=(vmem,) * 3,
        scratch_shapes=[
            pltpu.VMEM((fac_n, width), BF16),
            pltpu.VMEM((cols, width), BF16),
            pltpu.VMEM((fac_n // 128, 128), jnp.int32),
            pltpu.VMEM((demand.shape[0] // 128, 128), jnp.int32),
            pltpu.VMEM((fac_n // 128, 128), F32),
            pltpu.VMEM((fac_n // 128, 128), F32),
            pltpu.VMEM((fac_n // 128, 128), F32),
            pltpu.VMEM((demand.shape[0] // 128, 128), F32),
            dma((8,)),
            pltpu.VMEM((nz, half, width), BF16),
            pltpu.VMEM((nz, half, 128), BF16),
            pltpu.VMEM((ng, width + 128, cols), BF16),
            pltpu.VMEM((nz, 8, 128), F32),
            pltpu.VMEM((ng, 8, cols), F32),
            pltpu.VMEM((ny, CORES * crows, 128), F32),
            pltpu.VMEM((tall * half, cols), F32),
            pltpu.VMEM((tall * half, cols), F32),
            pltpu.VMEM((nz, half, 128), F32),
            pltpu.VMEM((ng, 8, cols), F32),
            pltpu.VMEM((8, 128), F32),
            pltpu.VMEM((ng, 8, cols), F32),
            pltpu.VMEM((ny, CORES * crows, 128), F32),
            pltpu.VMEM((hrows * nz, 128), F32),
            pltpu.VMEM((hrows * nz, 128), F32),
            pltpu.VMEM((hrows * nz, 128), F32),
            pltpu.VMEM((8, 128), F32),
            pltpu.VMEM((ITERS * ny, ng, CORES * crows, 128), F32),
            pltpu.VMEM((ITERS * groups, nx, 8, 128), F32),
            pltpu.VMEM((ITERS * groups, nz, 8, 128), F32),
            pltpu.VMEM((nz, ny * crows, 128), F32),
            pltpu.VMEM((ng, 8, 128), F32),
            dma((nz,)), dma((nz,)), dma(()), dma(()), dma((ng,)), dma((ng,)), dma((ny,)),
            dma((ITERS * ny,)), dma((ITERS * ny,)), dma((ITERS * groups,)), dma((ITERS * groups,)),
            dma((ITERS * groups,)), dma((ITERS * groups,)), dma(()), dma(()), dma(()), dma(()),
        ],
        compiler_params=pltpu.CompilerParams(
            collective_id=0,
            has_side_effects=True,
            vmem_limit_bytes=60 * 1024 * 1024,
        ),
        name="dual",
    )(
        fac_coords, cust_coords, view(open_flags), view(demand), view(fixed_cost), view(capacity),
        view(cap_mult), view(cover_mult),
    )
    return lam.reshape(-1), mu.reshape(-1), bounds[:ITERS, 0]


def solution(mesh, dims=(4, 8, 4)):
    return jax.shard_map(
        functools.partial(local, dims),
        mesh=mesh,
        in_specs=(
            P("fac", None),
            P(("cust", "fac"), None),
            P("fac"),
            P("cust"),
            P("fac"),
            P("fac"),
            P("fac"),
            P("cust"),
        ),
        out_specs=(P("cust"), P("fac"), P()),
        check_vma=False,
    )
```

```python
import functools
import math

import jax
import jax.numpy as jnp
from jax import lax
from jax.experimental import pallas as pl
from jax.experimental.pallas import tpu as pltpu
from jax.sharding import PartitionSpec as P

ITERS = 3
CORES = 2
TAU = 0.1
BIG = float(2**20)
LN2 = math.log(2.0)
MESH = pl.DeviceIdType.MESH
F32 = jnp.float32
BF16 = jnp.bfloat16


def split3(v):
    hi = v.astype(BF16).astype(F32)
    rest = v - hi
    mid = rest.astype(BF16).astype(F32)
    lo = (rest - mid).astype(BF16).astype(F32)
    return hi, mid, lo


def place_rows(shape, rows):
    at = lax.broadcasted_iota(jnp.int32, shape, 0)
    out = jnp.zeros(shape, F32)
    for index, row in rows.items():
        out = jnp.where(at == index, jnp.broadcast_to(row, shape), out)
    return out


def fold(v):
    total = v[:, :128]
    for j in range(1, v.shape[1] // 128):
        total = total + v[:, 128 * j : 128 * (j + 1)]
    return total


def kernel(
    ny, nz, nx, tall,
    fac_hbm, cust_hbm, flag_hbm, dem_hbm, fix_hbm, cap_hbm, mu_hbm, lam_hbm,
    lam_out, mu_out, bound_out,
    fac_ref, cust_ref, flag_ref, dem_ref, fix_ref, cap_ref, mu_ref, lam_ref, in_sem,
    fp, fx, r, fv, d8, dm, s0, s1, ld, cv, soft, lg, lam_s, mu_s, pn_s, cap_s, tt,
    cx, l1, l2, fin, tf,
    fp_send, fp_recv, fv_send, fv_recv, r_send, r_recv, fw_send,
    c_send, c_recv, l1_send, l1_recv, l2_send, l2_recv, fin_send, fin_recv, tf_send, tf_recv,
):
    ng = ny * CORES
    half = fac_ref.shape[0] // CORES
    cols = cust_ref.shape[0]
    width = fac_ref.shape[1]
    hrows = half // 128
    crows = cols // 128
    groups = nz // tall
    grows = tall * hrows
    total_cust = float(dem_ref.shape[0] * 128 * nx * CORES)
    f = lax.axis_index("fac")
    c = lax.axis_index("cust")
    y, z = f // nz, f % nz
    x, core = c // CORES, c % CORES
    g = y * CORES + core
    scale = math.log2(math.e) / (width * TAU)

    pairs = (
        (cust_hbm, cust_ref), (fac_hbm, fac_ref), (flag_hbm, flag_ref), (dem_hbm, dem_ref),
        (lam_hbm, lam_ref), (mu_hbm, mu_ref), (cap_hbm, cap_ref), (fix_hbm, fix_ref),
    )
    loads_in = [pltpu.make_async_copy(a, b, in_sem.at[n]) for n, (a, b) in enumerate(pairs)]
    for copy in loads_in:
        copy.start()

    def at(y_, z_, x_, core_):
        return (y_ * nz + z_, x_ * CORES + core_)

    def near(o, n):
        step = (o + 1) // 2
        return lax.rem(step * (2 * lax.rem(o, 2) - 1) + n, n)

    def z_at(o):
        return lax.rem(z + near(o, nz), nz)

    def y_at(o):
        return lax.rem(y + near(o, ny), ny)

    def z_dev(o):
        zp = z_at(o)
        return zp, at(y, zp, x, core)

    def g_dev(o):
        gp = lax.rem(g + o, ng)
        return gp, at(gp // CORES, z, x, lax.rem(gp, CORES))

    def z_plain(o):
        zp = lax.rem(z + o, nz)
        return zp, at(y, zp, x, core)

    def x_dev(o):
        xp = lax.rem(x + o, nx)
        return xp, at(y, z, xp, core)

    me = at(y, z, x, core)

    def remote(src, dst, send, recv, dev):
        return pltpu.make_async_remote_copy(
            src_ref=src, dst_ref=dst, send_sem=send, recv_sem=recv, device_id=dev, device_id_type=MESH
        )

    def loop(n, body, start=0):
        lax.fori_loop(start, n, lambda i, _: (body(jnp.int32(i)), 0)[1], 0)

    barrier = pltpu.get_barrier_semaphore()

    def greet(dev_of, n):
        def body(o):
            pl.semaphore_signal(barrier, inc=1, device_id=dev_of(o)[1], device_id_type=MESH)

        loop(n, body, 1)

    greet(z_dev, nz)
    greet(g_dev, ng)
    greet(x_dev, nx)

    def zero():
        def zero_rows(b):
            ld[b] = jnp.zeros((half, 128), F32)

        def zero_cols(s):
            cv[s] = jnp.zeros((8, cols), F32)
            lg[s] = jnp.zeros((8, cols), F32)

        loop(nz, zero_rows)
        loop(ng, zero_cols)

    def clear(s):
        r[s, width + 32 :, :] = jnp.zeros((r.shape[1] - width - 32, cols), BF16)

    loop(ng, clear)
    zero()
    tt[...] = jnp.zeros((8, 128), F32)
    soft[...] = jnp.zeros((8, 128), F32)
    for copy in loads_in:
        copy.wait()

    one = jnp.ones((1, 128), F32)
    for j in range(crows):
        lanes = slice(128 * j, 128 * (j + 1))
        qt = cust_ref[128 * j : 128 * (j + 1), :].astype(F32).T
        r[g, 0:width, lanes] = (2.0 * qt).astype(BF16)
        qn = jnp.sum(qt * qt, axis=0, keepdims=True)
        dem = dem_ref[pl.ds(f * crows + j, 1), :].astype(F32)
        lam0 = lam_ref[pl.ds(f * crows + j, 1), :]
        qh, qm, ql = split3(-qn)
        r[g, width : width + 16, lanes] = place_rows(
            (16, 128), {0: qh, 1: qm, 2: ql, 3: -one, 4: -one, 5: -one, 6: -dem, 7: -dem, 8: -dem}
        ).astype(BF16)
        lh, lm, ll = split3(width * lam0)
        r[g, width + 16 : width + 32, lanes] = place_rows((16, 128), {0: lh, 1: lm, 2: ll}).astype(BF16)

    mine = pl.ds(pl.multiple_of(core * half, half), half)
    opened = (flag_ref[pl.ds(core * hrows, hrows), :]).astype(F32)
    for j in range(hrows):
        pt = fac_ref[pl.ds(pl.multiple_of(core * half + 128 * j, 128), 128), :].astype(F32).T
        pn = jnp.sum(pt * pt, axis=0, keepdims=True)
        fv[z, j : j + 1, :] = pn + BIG * (1.0 - opened[j : j + 1])
    fv[z, hrows : 2 * hrows, :] = mu_ref[pl.ds(core * hrows, hrows), :]
    fv[z, 2 * hrows : 3 * hrows, :] = cap_ref[pl.ds(core * hrows, hrows), :]
    fv[z, 3 * hrows : 4 * hrows, :] = jnp.zeros((hrows, 128), F32)
    fp[z] = fac_ref[mine, :]

    pl.semaphore_wait(barrier, (nz - 1) + (ng - 1) + (nx - 1))

    chunk = pl.ds(0, width + 32)

    def fac_copy(o):
        zp, dev = z_dev(o)
        return remote(fac_ref.at[mine], fp.at[z], fp_send.at[zp], fp_recv.at[z], dev)

    def vec_copy(o):
        zp, dev = z_dev(o)
        return remote(fv.at[z], fv.at[z], fv_send, fv_recv, dev)

    def own_copy(o):
        yp = y_at(o)
        return remote(
            r.at[g, chunk], r.at[g, chunk], r_send.at[yp * CORES + core], r_recv.at[g], at(yp, z, x, core)
        )

    def forward(o):
        yp = y_at(o)
        s = yp * CORES + core
        return remote(r.at[s, chunk], r.at[s, chunk], fw_send.at[yp], r_recv.at[s], at(y, z, x, 1 - core))

    loop(nz, lambda o: vec_copy(o).start(), 1)
    loop(ny, lambda o: own_copy(o).start(), 1)
    forward(jnp.int32(0)).start()
    early = z < nz // 2

    @pl.when(early)
    def _():
        loop(nz, lambda o: fac_copy(o).start(), 1)


    def chunk_wait(s):
        remote(r.at[s, chunk], r.at[s, chunk], r_send.at[s], r_recv.at[s], me).wait_recv()

    def chunk_on(o):
        chunk_wait(y_at(o) * CORES + core)
        forward(o).start()

    def pair_in(o):
        pair = y_at(o)
        chunk_wait(pair * CORES + 1 - core)
        for h in range(CORES):
            s = pair * CORES + h
            extra = r[s, width : width + 16, :].astype(F32)
            dem = -extra[6:7]
            d8[s] = jnp.broadcast_to(dem, (8, cols))
            lam = r[s, width + 16 : width + 32, :].astype(F32)
            lam = (lam[0:1] + lam[1:2] + lam[2:3]) * (1.0 / width)
            for j in range(crows):
                row = h * crows + j
                dm[pair, row : row + 1, :] = dem[:, 128 * j : 128 * (j + 1)]
                lam_s[pair, row : row + 1, :] = lam[:, 128 * j : 128 * (j + 1)]

    def build_extra(b):
        for j in range(hrows):
            ph, pm, pll = split3(pn_s[pl.ds(b * hrows + j, 1), :])
            mh, mm, ml = split3(width * mu_s[pl.ds(b * hrows + j, 1), :])
            top = place_rows(
                (24, 128),
                {0: one, 1: one, 2: one, 3: ph, 4: pm, 5: pll, 6: mh, 7: mm, 8: ml, 16: one, 17: one, 18: one},
            )
            block = jnp.concatenate([top, jnp.zeros((104, 128), F32)], axis=0)
            fx[b, 128 * j : 128 * (j + 1), :] = block.T.astype(BF16)

    def vectors_in():
        others = fv.at[pl.ds(0, nz - 1)]
        remote(others, others, fv_send, fv_recv, me).wait_recv()
        for zp in range(nz):
            rows = slice(hrows * zp, hrows * (zp + 1))
            pn_s[rows, :] = fv[zp, 0:hrows, :]
            mu_s[rows, :] = fv[zp, hrows : 2 * hrows, :]
            cap_s[rows, :] = fv[zp, 2 * hrows : 3 * hrows, :]
        for zp in range(nz):
            build_extra(zp)

    def rows_in(group):
        for zp in range(group * tall, (group + 1) * tall):

            @pl.when(z != zp)
            def _():
                remote(fp.at[zp], fp.at[zp], fp_send.at[zp], fp_recv.at[zp], me).wait_recv()

    span = ng // 2
    turns = groups * span

    def place(k, i, h):
        group, pair = lax.rem(i // span, groups), lax.rem(i, span)
        if k == 0:
            pair = jnp.where(i < span, y_at(pair), pair)
        return group, pair * CORES + h

    def product(k, slot, i, h):
        group, s = place(k, i, h)
        blocks = pl.ds(group * tall, tall)
        rows = jnp.concatenate(
            [fp[blocks].reshape(tall * half, width), fx[blocks].reshape(tall * half, 128)], axis=1
        )
        slot[...] = jnp.dot(rows, r[s], preferred_element_type=F32)

    def pointwise(k, slot, i, h):
        group, s = place(k, i, h)
        cov = cv[s]
        logs = lg[s]
        dem = d8[s]
        prod, count = None, 0
        parts = tall * half // 8
        for n in range(parts):
            e = jnp.exp2(slot[8 * n : 8 * n + 8, :] * scale)
            u = 1.0 + e
            share = e / u
            cov = cov + share
            at_row = (8 * n) % half
            ld[group * tall + 8 * n // half, at_row : at_row + 8, :] += fold(share * dem)
            prod = u if prod is None else prod * u
            count += 1
            if count == 3 or n == parts - 1:
                logs = logs + jnp.log2(prod)
                prod, count = None, 0
        cv[s] = cov
        lg[s] = logs

    def part(ref, n, who):
        return ref.at[n, who] if n == ITERS * groups - 1 else ref.at[n, who, pl.ds(0, grows)]

    def l1_copy(n, o):
        xp, dev = x_dev(o)
        return remote(part(l1, n, x), part(l1, n, x), l1_send.at[n], l1_recv.at[n], dev)

    def l2_copy(n, o):
        zp, dev = z_plain(o)
        return remote(part(l2, n, z), part(l2, n, z), l2_send.at[n], l2_recv.at[n], dev)

    def c_copy(n, o):
        gp, dev = g_dev(o)
        return remote(cx.at[n, g], cx.at[n, g], c_send.at[n], c_recv.at[n], dev)

    def fin_copy(o):
        zp, dev = z_plain(o)
        return remote(fin.at[z], fin.at[z], fin_send, fin_recv, dev)

    def all_of(ref, n, count, send, recv):
        others = ref.at[n, pl.ds(0, count - 1)] if ref is cx else part(ref, n, pl.ds(0, count - 1))
        return remote(others, others, send.at[n], recv.at[n], me)

    def loads_out(k, group):
        n = k * groups + group
        rows = []
        for b in range(group * tall, (group + 1) * tall):
            for j in range(hrows):
                block = ld[b, 128 * j : 128 * (j + 1), :].T
                rows.append(jnp.sum(block, axis=0, keepdims=True))
        l1[n, x, 0:grows, :] = jnp.concatenate(rows, axis=0)
        if n == ITERS * groups - 1:
            l1[n, x, grows:, :] = tt[...]
        loop(nx, lambda o: l1_copy(n, o).start(), 1)
        for b in range(group * tall, (group + 1) * tall):
            ld[b] = jnp.zeros((half, 128), F32)

    def loads_on(k, group):
        n = k * groups + group
        all_of(l1, n, nx, l1_send, l1_recv).wait_recv()
        end = l1.shape[2] if n == ITERS * groups - 1 else grows
        total = l1[n, 0, 0:end, :]
        for xp in range(1, nx):
            total = total + l1[n, xp, 0:end, :]
        l2[n, z, 0:end, :] = total
        loop(nz, lambda o: l2_copy(n, o).start(), 1)

    def loads_in_use(k, group):
        n = k * groups + group
        all_of(l2, n, nz, l2_send, l2_recv).wait_recv()
        end = l2.shape[2] if n == ITERS * groups - 1 else grows
        whole = l2[n, 0, 0:end, :]
        for zp in range(1, nz):
            whole = whole + l2[n, zp, 0:end, :]
        load = whole[:grows]
        rows = slice(group * grows, (group + 1) * grows)
        cap = cap_s[rows, :]
        size = 0.1 / (k + 1)
        mu_s[rows, :] = jnp.maximum(0.0, mu_s[rows, :] + size * (load - cap) / (load + cap))
        if k < ITERS - 1:
            for b in range(group * tall, (group + 1) * tall):
                build_extra(b)
        elif group == groups - 1:
            tf[g] = whole[grows:]

    def cover_out(k, pair):
        n = k * ny + pair
        rows = []
        for s in range(pair * CORES, (pair + 1) * CORES):
            cov = jnp.sum(cv[s], axis=0, keepdims=True)
            rows += [cov[:, 128 * j : 128 * (j + 1)] for j in range(crows)]
        cx[n, g] = jnp.concatenate(rows, axis=0)
        loop(ng, lambda o: c_copy(n, o).start(), 1)
        total = soft[...]
        for s in range(pair * CORES, (pair + 1) * CORES):
            total = total + fold(lg[s] * d8[s])
            cv[s] = jnp.zeros((8, cols), F32)
            lg[s] = jnp.zeros((8, cols), F32)
        soft[...] = total
        if pair == ny - 1:
            tt[k : k + 1, :] = tt[k : k + 1, :] - (TAU * LN2) * jnp.sum(total, axis=0, keepdims=True)
            soft[...] = jnp.zeros((8, 128), F32)

    def cover_in_use(k, pair):
        n = k * ny + pair
        all_of(cx, n, ng, c_send, c_recv).wait_recv()
        cover = cx[n, 0]
        for gp in range(1, ng):
            cover = cover + cx[n, gp]
        size = 0.1 / (k + 1)
        lam = lam_s[pair] + size * dm[pair] * (1.0 - cover) / (1.0 + cover)
        lam_s[pair] = lam
        if k < ITERS - 1:
            lh, lm, ll = split3(width * lam)
            for m in range(CORES * crows):
                s, j = pair * CORES + m // crows, m % crows
                r[s, width + 16 : width + 32, 128 * j : 128 * (j + 1)] = place_rows(
                    (16, 128), {0: lh[m : m + 1], 1: lm[m : m + 1], 2: ll[m : m + 1]}
                ).astype(BF16)

    def terms(k):
        mine_rows = pl.ds(core * crows, crows)
        priced = jnp.sum(lam_s[y, mine_rows, :] * dm[y, mine_rows, :], axis=0, keepdims=True)
        own = pl.ds(z * hrows, hrows)
        rowterm = opened * fix_ref[pl.ds(core * hrows, hrows), :] - mu_s[own, :] * cap_s[own, :]
        tt[k : k + 1, :] = priced + jnp.sum(rowterm, axis=0, keepdims=True) * (1.0 / nx)

    def events(k, i):
        def when(turn, *jobs):
            @pl.when(i == turn)
            def _():
                for job in jobs:
                    job()

        job = functools.partial
        last = groups - 1
        table = {}

        def add(turn, fn, step_of, *args):
            if turn // turns + step_of == k:
                table.setdefault(turn % turns, []).append(job(fn, step_of, *args))

        for of in range(max(k - 1, 0), k + 1):
            for pair in range(ny):
                add(span * last + 1 + pair, cover_out, of, pair)
            for group in range(groups):
                add(span * (group + 1), loads_out, of, group)
        for of in range(max(k - 1, 0), k + 1):
            add(turns - 2, terms, of)
            for group in range(groups):
                add(span * (group + 1) + 1, loads_on, of, group)
        for of in range(max(k - 1, 0), k + 1):
            for group in range(groups):
                add(span * (group + 1) + 3, loads_in_use, of, group)
            if of < ITERS - 1:
                for pair in range(ny):
                    add(turns - 1 + pair, cover_in_use, of, pair)
        if k == 0:
            def sent(_):
                loop(nz, lambda o: fac_copy(o).wait_send(), 1)
                loop(ny, lambda o: own_copy(o).wait_send(), 1)
                loop(ny, lambda o: forward(o).wait_send())

            add(turns - 2, sent, 0)
            for group in range(1, groups):
                add(span * group - 1, lambda _, n=group: rows_in(n), 0)
        for turn in sorted(table):
            when(turn, *table[turn])

    def step(k):
        def two(i):
            if k == 0:

                @pl.when(i == 1)
                def _():
                    for o in range(3, ny):
                        chunk_on(jnp.int32(o))

                @pl.when(i + 1 < span)
                def _():
                    pair_in(i + 1)

            events(k, i)
            product(k, s1, i, 1)
            pointwise(k, s0, i, 0)
            product(k, s0, i + 1, 0)
            pointwise(k, s1, i, 1)

        loop(turns, two)

    vectors_in()
    pair_in(jnp.int32(0))

    @pl.when(jnp.logical_not(early))
    def _():
        loop(nz, lambda o: fac_copy(o).start(), 1)

    rows_in(0)
    for o in range(1, min(3, ny)):
        chunk_on(jnp.int32(o))
    product(0, s0, jnp.int32(0), 0)
    for k in range(ITERS):
        step(k)

    k, last = ITERS - 1, groups - 1
    cover_out(k, ny - 1)
    loads_out(k, last)
    for group in range(last):
        if span * (group + 1) + 3 >= turns:
            loads_in_use(k, group)
    loads_on(k, last)
    for pair in range(ny):
        cover_in_use(k, pair)
    for yp in range(ny):
        fin[z, yp * crows : (yp + 1) * crows, :] = lam_s[yp, pl.ds(core * crows, crows), :]
    loop(nz, lambda o: fin_copy(o).start(), 1)
    for n in range(ITERS * groups):
        all_of(l1, n, nx, l1_send, l1_recv).wait_send()
    for n in range(ITERS * ny):
        all_of(cx, n, ng, c_send, c_recv).wait_send()
    remote(fv.at[pl.ds(0, nz - 1)], fv.at[pl.ds(0, nz - 1)], fv_send, fv_recv, me).wait_send()
    loads_in_use(k, last)

    tf[g, ITERS : ITERS + hrows, :] = mu_s[pl.ds(z * hrows, hrows), :]

    def tf_copy(o):
        gp, dev = g_dev(o)
        return remote(tf.at[g], tf.at[g], tf_send, tf_recv, dev)

    loop(ng, lambda o: tf_copy(o).start(), 1)

    others = fin.at[pl.ds(0, nz - 1)]
    remote(others, others, fin_send, fin_recv, me).wait_recv()
    for yp in range(ny):
        for zp in range(nz):
            first = (yp * nz + zp) * crows
            lam_out[first : first + crows, :] = fin[zp, yp * crows : (yp + 1) * crows, :]
    for n in range(ITERS * groups):
        all_of(l2, n, nz, l2_send, l2_recv).wait_send()
    remote(others, others, fin_send, fin_recv, me).wait_send()
    peers = tf.at[pl.ds(0, ng - 1)]
    remote(peers, peers, tf_send, tf_recv, me).wait_recv()
    total = tf[0]
    for gp in range(1, ng):
        total = total + tf[gp]
    sums = jnp.sum(total, axis=1, keepdims=True) * (1.0 / total_cust)
    bound_out[...] = jnp.broadcast_to(sums, (8, 128))
    for h in range(CORES):
        mu_out[h * hrows : (h + 1) * hrows, :] = tf[y * CORES + h, ITERS : ITERS + hrows, :]
    remote(peers, peers, tf_send, tf_recv, me).wait_send()


def local(dims, fac_coords, cust_coords, open_flags, demand, fixed_cost, capacity, cap_mult, cover_mult):
    ny, nz, nx = dims
    ng = ny * CORES
    fac_n, width = fac_coords.shape
    half = fac_n // CORES
    cols = cust_coords.shape[0]
    hrows = half // 128
    crows = cols // 128
    view = lambda a: a.reshape(-1, 128)
    vmem = pl.BlockSpec(memory_space=pltpu.VMEM)
    hbm = pl.BlockSpec(memory_space=pltpu.HBM)
    tall = 4
    groups = nz // tall
    dma = pltpu.SemaphoreType.DMA
    lam, mu, bounds = pl.pallas_call(
        functools.partial(kernel, ny, nz, nx, tall),
        out_shape=(
            jax.ShapeDtypeStruct((demand.shape[0] // 128, 128), F32),
            jax.ShapeDtypeStruct((fac_n // 128, 128), F32),
            jax.ShapeDtypeStruct((8, 128), F32),
        ),
        in_specs=[hbm] * 8,
        out_specs=(vmem,) * 3,
        scratch_shapes=[
            pltpu.VMEM((fac_n, width), BF16),
            pltpu.VMEM((cols, width), BF16),
            pltpu.VMEM((fac_n // 128, 128), jnp.int32),
            pltpu.VMEM((demand.shape[0] // 128, 128), jnp.int32),
            pltpu.VMEM((fac_n // 128, 128), F32),
            pltpu.VMEM((fac_n // 128, 128), F32),
            pltpu.VMEM((fac_n // 128, 128), F32),
            pltpu.VMEM((demand.shape[0] // 128, 128), F32),
            dma((8,)),
            pltpu.VMEM((nz, half, width), BF16),
            pltpu.VMEM((nz, half, 128), BF16),
            pltpu.VMEM((ng, width + 128, cols), BF16),
            pltpu.VMEM((nz, 8, 128), F32),
            pltpu.VMEM((ng, 8, cols), F32),
            pltpu.VMEM((ny, CORES * crows, 128), F32),
            pltpu.VMEM((tall * half, cols), F32),
            pltpu.VMEM((tall * half, cols), F32),
            pltpu.VMEM((nz, half, 128), F32),
            pltpu.VMEM((ng, 8, cols), F32),
            pltpu.VMEM((8, 128), F32),
            pltpu.VMEM((ng, 8, cols), F32),
            pltpu.VMEM((ny, CORES * crows, 128), F32),
            pltpu.VMEM((hrows * nz, 128), F32),
            pltpu.VMEM((hrows * nz, 128), F32),
            pltpu.VMEM((hrows * nz, 128), F32),
            pltpu.VMEM((8, 128), F32),
            pltpu.VMEM((ITERS * ny, ng, CORES * crows, 128), F32),
            pltpu.VMEM((ITERS * groups, nx, tall * hrows + 8, 128), F32),
            pltpu.VMEM((ITERS * groups, nz, tall * hrows + 8, 128), F32),
            pltpu.VMEM((nz, ny * crows, 128), F32),
            pltpu.VMEM((ng, 8, 128), F32),
            dma((nz,)), dma((nz,)), dma(()), dma(()), dma((ng,)), dma((ng,)), dma((ny,)),
            dma((ITERS * ny,)), dma((ITERS * ny,)), dma((ITERS * groups,)), dma((ITERS * groups,)),
            dma((ITERS * groups,)), dma((ITERS * groups,)), dma(()), dma(()), dma(()), dma(()),
        ],
        compiler_params=pltpu.CompilerParams(
            collective_id=0,
            has_side_effects=True,
            vmem_limit_bytes=60 * 1024 * 1024,
        ),
        name="dual",
    )(
        fac_coords, cust_coords, view(open_flags), view(demand), view(fixed_cost), view(capacity),
        view(cap_mult), view(cover_mult),
    )
    return lam.reshape(-1), mu.reshape(-1), bounds[:ITERS, 0]


def solution(mesh, dims=(4, 8, 4)):
    return jax.shard_map(
        functools.partial(local, dims),
        mesh=mesh,
        in_specs=(
            P("fac", None),
            P(("cust", "fac"), None),
            P("fac"),
            P("cust"),
            P("fac"),
            P("fac"),
            P("fac"),
            P("cust"),
        ),
        out_specs=(P("cust"), P("fac"), P()),
        check_vma=False,
    )
```

```python
import functools
import math

import jax
import jax.numpy as jnp
from jax import lax
from jax.experimental import pallas as pl
from jax.experimental.pallas import tpu as pltpu
from jax.sharding import PartitionSpec as P

ITERS = 3
CORES = 2
TAU = 0.1
BIG = float(2**20)
LN2 = math.log(2.0)
MESH = pl.DeviceIdType.MESH
F32 = jnp.float32
BF16 = jnp.bfloat16


def split3(v):
    hi = v.astype(BF16).astype(F32)
    rest = v - hi
    mid = rest.astype(BF16).astype(F32)
    lo = (rest - mid).astype(BF16).astype(F32)
    return hi, mid, lo


def place_rows(shape, rows):
    at = lax.broadcasted_iota(jnp.int32, shape, 0)
    out = jnp.zeros(shape, F32)
    for index, row in rows.items():
        out = jnp.where(at == index, jnp.broadcast_to(row, shape), out)
    return out


def fold(v):
    total = v[:, :128]
    for j in range(1, v.shape[1] // 128):
        total = total + v[:, 128 * j : 128 * (j + 1)]
    return total


def kernel(
    ny, nz, nx, tall,
    fac_hbm, cust_hbm, flag_hbm, dem_hbm, fix_hbm, cap_hbm, mu_hbm, lam_hbm,
    lam_out, mu_out, bound_out,
    fac_ref, cust_ref, flag_ref, dem_ref, fix_ref, cap_ref, mu_ref, lam_ref, in_sem,
    fp, fx, r, fv, d8, dm, s0, s1, ld, cv, soft, lg, lam_s, mu_s, pn_s, cap_s, tt,
    cx, l1, l2, fin, tf,
    fp_send, fp_recv, fv_send, fv_recv, r_send, r_recv, fw_send,
    c_send, c_recv, l1_send, l1_recv, l2_send, l2_recv, fin_send, fin_recv, tf_send, tf_recv,
):
    ng = ny * CORES
    half = fac_ref.shape[0] // CORES
    cols = cust_ref.shape[0]
    width = fac_ref.shape[1]
    hrows = half // 128
    crows = cols // 128
    groups = nz // tall
    grows = tall * hrows
    total_cust = float(dem_ref.shape[0] * 128 * nx * CORES)
    f = lax.axis_index("fac")
    c = lax.axis_index("cust")
    y, z = f // nz, f % nz
    x, core = c // CORES, c % CORES
    g = y * CORES + core
    scale = math.log2(math.e) / (width * TAU)

    pairs = (
        (cust_hbm, cust_ref), (fac_hbm, fac_ref), (flag_hbm, flag_ref), (dem_hbm, dem_ref),
        (lam_hbm, lam_ref), (mu_hbm, mu_ref), (cap_hbm, cap_ref), (fix_hbm, fix_ref),
    )
    loads_in = [pltpu.make_async_copy(a, b, in_sem.at[n]) for n, (a, b) in enumerate(pairs)]
    for copy in loads_in:
        copy.start()

    def at(y_, z_, x_, core_):
        return (y_ * nz + z_, x_ * CORES + core_)

    def near(o, n):
        step = (o + 1) // 2
        return lax.rem(step * (2 * lax.rem(o, 2) - 1) + n, n)

    def z_at(o):
        return lax.rem(z + near(o, nz), nz)

    def y_at(o):
        return lax.rem(y + near(o, ny), ny)

    def z_dev(o):
        zp = z_at(o)
        return zp, at(y, zp, x, core)

    def g_dev(o):
        gp = lax.rem(g + o, ng)
        return gp, at(gp // CORES, z, x, lax.rem(gp, CORES))

    def z_plain(o):
        zp = lax.rem(z + o, nz)
        return zp, at(y, zp, x, core)

    def x_dev(o):
        xp = lax.rem(x + o, nx)
        return xp, at(y, z, xp, core)

    me = at(y, z, x, core)

    def remote(src, dst, send, recv, dev):
        return pltpu.make_async_remote_copy(
            src_ref=src, dst_ref=dst, send_sem=send, recv_sem=recv, device_id=dev, device_id_type=MESH
        )

    def loop(n, body, start=0):
        lax.fori_loop(start, n, lambda i, _: (body(jnp.int32(i)), 0)[1], 0)

    barrier = pltpu.get_barrier_semaphore()

    def greet(dev_of, n):
        def body(o):
            pl.semaphore_signal(barrier, inc=1, device_id=dev_of(o)[1], device_id_type=MESH)

        loop(n, body, 1)

    greet(z_dev, nz)
    greet(g_dev, ng)
    greet(x_dev, nx)

    def zero():
        def zero_rows(b):
            ld[b] = jnp.zeros((half, 128), F32)

        def zero_cols(s):
            cv[s] = jnp.zeros((8, cols), F32)
            lg[s] = jnp.zeros((8, cols), F32)

        loop(nz, zero_rows)
        loop(ng, zero_cols)

    def clear(s):
        r[s, width + 32 :, :] = jnp.zeros((r.shape[1] - width - 32, cols), BF16)

    loop(ng, clear)
    zero()
    tt[...] = jnp.zeros((8, 128), F32)
    soft[...] = jnp.zeros((8, 128), F32)
    for copy in loads_in:
        copy.wait()

    one = jnp.ones((1, 128), F32)
    for j in range(crows):
        lanes = slice(128 * j, 128 * (j + 1))
        qt = cust_ref[128 * j : 128 * (j + 1), :].astype(F32).T
        r[g, 0:width, lanes] = (2.0 * qt).astype(BF16)
        qn = jnp.sum(qt * qt, axis=0, keepdims=True)
        dem = dem_ref[pl.ds(f * crows + j, 1), :].astype(F32)
        lam0 = lam_ref[pl.ds(f * crows + j, 1), :]
        qh, qm, ql = split3(-qn)
        r[g, width : width + 16, lanes] = place_rows(
            (16, 128), {0: qh, 1: qm, 2: ql, 3: -one, 4: -one, 5: -one, 6: -dem, 7: -dem, 8: -dem}
        ).astype(BF16)
        lh, lm, ll = split3(width * lam0)
        r[g, width + 16 : width + 32, lanes] = place_rows((16, 128), {0: lh, 1: lm, 2: ll}).astype(BF16)

    mine = pl.ds(pl.multiple_of(core * half, half), half)
    opened = (flag_ref[pl.ds(core * hrows, hrows), :]).astype(F32)
    for j in range(hrows):
        pt = fac_ref[pl.ds(pl.multiple_of(core * half + 128 * j, 128), 128), :].astype(F32).T
        pn = jnp.sum(pt * pt, axis=0, keepdims=True)
        fv[z, j : j + 1, :] = pn + BIG * (1.0 - opened[j : j + 1])
    fv[z, hrows : 2 * hrows, :] = mu_ref[pl.ds(core * hrows, hrows), :]
    fv[z, 2 * hrows : 3 * hrows, :] = cap_ref[pl.ds(core * hrows, hrows), :]
    fv[z, 3 * hrows : 4 * hrows, :] = jnp.zeros((hrows, 128), F32)
    fp[z] = fac_ref[mine, :]

    pl.semaphore_wait(barrier, (nz - 1) + (ng - 1) + (nx - 1))

    chunk = pl.ds(0, width + 32)

    def fac_copy(o):
        zp, dev = z_dev(o)
        return remote(fac_ref.at[mine], fp.at[z], fp_send.at[zp], fp_recv.at[z], dev)

    def vec_copy(o):
        zp, dev = z_dev(o)
        return remote(fv.at[z], fv.at[z], fv_send, fv_recv, dev)

    def own_copy(o):
        yp = y_at(o)
        return remote(
            r.at[g, chunk], r.at[g, chunk], r_send.at[yp * CORES + core], r_recv.at[g], at(yp, z, x, core)
        )

    def forward(o):
        yp = y_at(o)
        s = yp * CORES + core
        return remote(r.at[s, chunk], r.at[s, chunk], fw_send.at[yp], r_recv.at[s], at(y, z, x, 1 - core))

    loop(nz, lambda o: vec_copy(o).start(), 1)
    loop(ny, lambda o: own_copy(o).start(), 1)
    forward(jnp.int32(0)).start()
    early = z < nz // 2

    @pl.when(early)
    def _():
        loop(nz, lambda o: fac_copy(o).start(), 1)


    def chunk_wait(s):
        remote(r.at[s, chunk], r.at[s, chunk], r_send.at[s], r_recv.at[s], me).wait_recv()

    def chunk_on(o):
        chunk_wait(y_at(o) * CORES + core)
        forward(o).start()

    def pair_in(o):
        pair = y_at(o)
        chunk_wait(pair * CORES + 1 - core)
        for h in range(CORES):
            s = pair * CORES + h
            extra = r[s, width : width + 16, :].astype(F32)
            dem = -extra[6:7]
            d8[s] = jnp.broadcast_to(dem, (8, cols))
            lam = r[s, width + 16 : width + 32, :].astype(F32)
            lam = (lam[0:1] + lam[1:2] + lam[2:3]) * (1.0 / width)
            for j in range(crows):
                row = h * crows + j
                dm[pair, row : row + 1, :] = dem[:, 128 * j : 128 * (j + 1)]
                lam_s[pair, row : row + 1, :] = lam[:, 128 * j : 128 * (j + 1)]

    def build_extra(b):
        for j in range(hrows):
            ph, pm, pll = split3(pn_s[pl.ds(b * hrows + j, 1), :])
            mh, mm, ml = split3(width * mu_s[pl.ds(b * hrows + j, 1), :])
            top = place_rows(
                (24, 128),
                {0: one, 1: one, 2: one, 3: ph, 4: pm, 5: pll, 6: mh, 7: mm, 8: ml, 16: one, 17: one, 18: one},
            )
            block = jnp.concatenate([top, jnp.zeros((104, 128), F32)], axis=0)
            fx[b, 128 * j : 128 * (j + 1), :] = block.T.astype(BF16)

    def vectors_in():
        others = fv.at[pl.ds(0, nz - 1)]
        remote(others, others, fv_send, fv_recv, me).wait_recv()
        for zp in range(nz):
            rows = slice(hrows * zp, hrows * (zp + 1))
            pn_s[rows, :] = fv[zp, 0:hrows, :]
            mu_s[rows, :] = fv[zp, hrows : 2 * hrows, :]
            cap_s[rows, :] = fv[zp, 2 * hrows : 3 * hrows, :]
        for zp in range(nz):
            build_extra(zp)

    def rows_in(group):
        for zp in range(group * tall, (group + 1) * tall):

            @pl.when(z != zp)
            def _():
                remote(fp.at[zp], fp.at[zp], fp_send.at[zp], fp_recv.at[zp], me).wait_recv()

    span = ng // 2
    turns = groups * span

    def place(k, i, h):
        group, pair = lax.rem(i // span, groups), lax.rem(i, span)
        if k == 0:
            pair = jnp.where(i < span, y_at(pair), pair)
        return group, pair * CORES + h

    def product(k, slot, i, h):
        group, s = place(k, i, h)
        blocks = pl.ds(group * tall, tall)
        rows = jnp.concatenate(
            [fp[blocks].reshape(tall * half, width), fx[blocks].reshape(tall * half, 128)], axis=1
        )
        slot[...] = jnp.dot(rows, r[s], preferred_element_type=F32)

    def pointwise(k, slot, i, h):
        group, s = place(k, i, h)
        cov = cv[s]
        logs = lg[s]
        dem = d8[s]
        prod, count = None, 0
        parts = tall * half // 8
        for n in range(parts):
            e = jnp.exp2(slot[8 * n : 8 * n + 8, :] * scale)
            u = 1.0 + e
            share = e / u
            cov = cov + share
            at_row = (8 * n) % half
            ld[group * tall + 8 * n // half, at_row : at_row + 8, :] += fold(share * dem)
            prod = u if prod is None else prod * u
            count += 1
            if count == 3 or n == parts - 1:
                logs = logs + jnp.log2(prod)
                prod, count = None, 0
        cv[s] = cov
        lg[s] = logs

    def part(ref, n, who):
        return ref.at[n, who] if n == ITERS * groups - 1 else ref.at[n, who, pl.ds(0, grows)]

    def l1_copy(n, o):
        xp, dev = x_dev(o)
        return remote(part(l1, n, x), part(l1, n, x), l1_send.at[n], l1_recv.at[n], dev)

    def l2_copy(n, o):
        zp, dev = z_plain(o)
        return remote(part(l2, n, z), part(l2, n, z), l2_send.at[n], l2_recv.at[n], dev)

    def c_copy(n, o):
        gp, dev = g_dev(o)
        return remote(cx.at[n, g], cx.at[n, g], c_send.at[n], c_recv.at[n], dev)

    def fin_copy(o):
        zp, dev = z_plain(o)
        return remote(fin.at[z], fin.at[z], fin_send, fin_recv, dev)

    def all_of(ref, n, count, send, recv):
        others = ref.at[n, pl.ds(0, count - 1)] if ref is cx else part(ref, n, pl.ds(0, count - 1))
        return remote(others, others, send.at[n], recv.at[n], me)

    def loads_out(k, group):
        n = k * groups + group
        rows = []
        for b in range(group * tall, (group + 1) * tall):
            for j in range(hrows):
                block = ld[b, 128 * j : 128 * (j + 1), :].T
                rows.append(jnp.sum(block, axis=0, keepdims=True))
        l1[n, x, 0:grows, :] = jnp.concatenate(rows, axis=0)
        if n == ITERS * groups - 1:
            l1[n, x, grows:, :] = tt[...]
        for o in range(1, nx):
            l1_copy(n, o).start()
        for b in range(group * tall, (group + 1) * tall):
            ld[b] = jnp.zeros((half, 128), F32)

    def loads_on(k, group):
        n = k * groups + group
        all_of(l1, n, nx, l1_send, l1_recv).wait_recv()
        end = l1.shape[2] if n == ITERS * groups - 1 else grows
        total = l1[n, 0, 0:end, :]
        for xp in range(1, nx):
            total = total + l1[n, xp, 0:end, :]
        l2[n, z, 0:end, :] = total
        for o in range(1, nz):
            l2_copy(n, o).start()

    def loads_in_use(k, group):
        n = k * groups + group
        all_of(l2, n, nz, l2_send, l2_recv).wait_recv()
        end = l2.shape[2] if n == ITERS * groups - 1 else grows
        whole = l2[n, 0, 0:end, :]
        for zp in range(1, nz):
            whole = whole + l2[n, zp, 0:end, :]
        load = whole[:grows]
        rows = slice(group * grows, (group + 1) * grows)
        cap = cap_s[rows, :]
        size = 0.1 / (k + 1)
        mu_s[rows, :] = jnp.maximum(0.0, mu_s[rows, :] + size * (load - cap) / (load + cap))
        if k < ITERS - 1:
            for b in range(group * tall, (group + 1) * tall):
                build_extra(b)
        elif group == groups - 1:
            tf[g] = whole[grows:]

    def cover_out(k, pair):
        n = k * ny + pair
        rows = []
        for s in range(pair * CORES, (pair + 1) * CORES):
            cov = jnp.sum(cv[s], axis=0, keepdims=True)
            rows += [cov[:, 128 * j : 128 * (j + 1)] for j in range(crows)]
        cx[n, g] = jnp.concatenate(rows, axis=0)
        for o in range(1, ng):
            c_copy(n, o).start()
        total = soft[...]
        for s in range(pair * CORES, (pair + 1) * CORES):
            total = total + fold(lg[s] * d8[s])
            cv[s] = jnp.zeros((8, cols), F32)
            lg[s] = jnp.zeros((8, cols), F32)
        soft[...] = total
        if pair == ny - 1:
            tt[k : k + 1, :] = tt[k : k + 1, :] - (TAU * LN2) * jnp.sum(total, axis=0, keepdims=True)
            soft[...] = jnp.zeros((8, 128), F32)

    def cover_in_use(k, pair):
        n = k * ny + pair
        all_of(cx, n, ng, c_send, c_recv).wait_recv()
        cover = cx[n, 0]
        for gp in range(1, ng):
            cover = cover + cx[n, gp]
        size = 0.1 / (k + 1)
        lam = lam_s[pair] + size * dm[pair] * (1.0 - cover) / (1.0 + cover)
        lam_s[pair] = lam
        if k < ITERS - 1:
            lh, lm, ll = split3(width * lam)
            for m in range(CORES * crows):
                s, j = pair * CORES + m // crows, m % crows
                r[s, width + 16 : width + 32, 128 * j : 128 * (j + 1)] = place_rows(
                    (16, 128), {0: lh[m : m + 1], 1: lm[m : m + 1], 2: ll[m : m + 1]}
                ).astype(BF16)

    def terms(k):
        mine_rows = pl.ds(core * crows, crows)
        priced = jnp.sum(lam_s[y, mine_rows, :] * dm[y, mine_rows, :], axis=0, keepdims=True)
        own = pl.ds(z * hrows, hrows)
        rowterm = opened * fix_ref[pl.ds(core * hrows, hrows), :] - mu_s[own, :] * cap_s[own, :]
        tt[k : k + 1, :] = priced + jnp.sum(rowterm, axis=0, keepdims=True) * (1.0 / nx)

    def events(k, i):
        def when(turn, *jobs):
            @pl.when(i == turn)
            def _():
                for job in jobs:
                    job()

        job = functools.partial
        last = groups - 1
        table = {}

        def add(turn, fn, step_of, *args):
            if turn // turns + step_of == k:
                table.setdefault(turn % turns, []).append(job(fn, step_of, *args))

        for of in range(max(k - 1, 0), k + 1):
            for pair in range(ny):
                add(span * last + 1 + pair, cover_out, of, pair)
            for group in range(groups):
                add(span * (group + 1), loads_out, of, group)
        for of in range(max(k - 1, 0), k + 1):
            add(turns - 2, terms, of)
            for group in range(groups):
                add(span * (group + 1) + 1, loads_on, of, group)
        for of in range(max(k - 1, 0), k + 1):
            for group in range(groups):
                add(span * (group + 1) + 3, loads_in_use, of, group)
            if of < ITERS - 1:
                for pair in range(ny):
                    add(turns - 1 + pair, cover_in_use, of, pair)
        if k == 0:
            def sent(_):
                loop(nz, lambda o: fac_copy(o).wait_send(), 1)
                loop(ny, lambda o: own_copy(o).wait_send(), 1)
                loop(ny, lambda o: forward(o).wait_send())

            add(turns - 2, sent, 0)
            for group in range(1, groups):
                add(span * group - 1, lambda _, n=group: rows_in(n), 0)
        for turn in sorted(table):
            when(turn, *table[turn])

    def step(k):
        def two(i):
            if k == 0:

                @pl.when(i == 1)
                def _():
                    for o in range(3, ny):
                        chunk_on(jnp.int32(o))

                @pl.when(i + 1 < span)
                def _():
                    pair_in(i + 1)

            events(k, i)
            product(k, s1, i, 1)
            pointwise(k, s0, i, 0)
            product(k, s0, i + 1, 0)
            pointwise(k, s1, i, 1)

        loop(turns, two)

    vectors_in()
    pair_in(jnp.int32(0))

    @pl.when(jnp.logical_not(early))
    def _():
        loop(nz, lambda o: fac_copy(o).start(), 1)

    rows_in(0)
    for o in range(1, min(3, ny)):
        chunk_on(jnp.int32(o))
    product(0, s0, jnp.int32(0), 0)
    for k in range(ITERS):
        step(k)

    k, last = ITERS - 1, groups - 1
    cover_out(k, ny - 1)
    loads_out(k, last)
    for group in range(last):
        if span * (group + 1) + 3 >= turns:
            loads_in_use(k, group)
    loads_on(k, last)
    for pair in range(ny):
        cover_in_use(k, pair)
    for yp in range(ny):
        fin[z, yp * crows : (yp + 1) * crows, :] = lam_s[yp, pl.ds(core * crows, crows), :]
    loop(nz, lambda o: fin_copy(o).start(), 1)
    for n in range(ITERS * groups):
        all_of(l1, n, nx, l1_send, l1_recv).wait_send()
    for n in range(ITERS * ny):
        all_of(cx, n, ng, c_send, c_recv).wait_send()
    remote(fv.at[pl.ds(0, nz - 1)], fv.at[pl.ds(0, nz - 1)], fv_send, fv_recv, me).wait_send()
    loads_in_use(k, last)

    tf[g, ITERS : ITERS + hrows, :] = mu_s[pl.ds(z * hrows, hrows), :]

    def tf_copy(o):
        gp, dev = g_dev(o)
        return remote(tf.at[g], tf.at[g], tf_send, tf_recv, dev)

    loop(ng, lambda o: tf_copy(o).start(), 1)

    others = fin.at[pl.ds(0, nz - 1)]
    remote(others, others, fin_send, fin_recv, me).wait_recv()
    for yp in range(ny):
        for zp in range(nz):
            first = (yp * nz + zp) * crows
            lam_out[first : first + crows, :] = fin[zp, yp * crows : (yp + 1) * crows, :]
    for n in range(ITERS * groups):
        all_of(l2, n, nz, l2_send, l2_recv).wait_send()
    remote(others, others, fin_send, fin_recv, me).wait_send()
    peers = tf.at[pl.ds(0, ng - 1)]
    remote(peers, peers, tf_send, tf_recv, me).wait_recv()
    total = tf[0]
    for gp in range(1, ng):
        total = total + tf[gp]
    sums = jnp.sum(total, axis=1, keepdims=True) * (1.0 / total_cust)
    bound_out[...] = jnp.broadcast_to(sums, (8, 128))
    for h in range(CORES):
        mu_out[h * hrows : (h + 1) * hrows, :] = tf[y * CORES + h, ITERS : ITERS + hrows, :]
    remote(peers, peers, tf_send, tf_recv, me).wait_send()


def local(dims, fac_coords, cust_coords, open_flags, demand, fixed_cost, capacity, cap_mult, cover_mult):
    ny, nz, nx = dims
    ng = ny * CORES
    fac_n, width = fac_coords.shape
    half = fac_n // CORES
    cols = cust_coords.shape[0]
    hrows = half // 128
    crows = cols // 128
    view = lambda a: a.reshape(-1, 128)
    vmem = pl.BlockSpec(memory_space=pltpu.VMEM)
    hbm = pl.BlockSpec(memory_space=pltpu.HBM)
    tall = 4
    groups = nz // tall
    dma = pltpu.SemaphoreType.DMA
    lam, mu, bounds = pl.pallas_call(
        functools.partial(kernel, ny, nz, nx, tall),
        out_shape=(
            jax.ShapeDtypeStruct((demand.shape[0] // 128, 128), F32),
            jax.ShapeDtypeStruct((fac_n // 128, 128), F32),
            jax.ShapeDtypeStruct((8, 128), F32),
        ),
        in_specs=[hbm] * 8,
        out_specs=(vmem,) * 3,
        scratch_shapes=[
            pltpu.VMEM((fac_n, width), BF16),
            pltpu.VMEM((cols, width), BF16),
            pltpu.VMEM((fac_n // 128, 128), jnp.int32),
            pltpu.VMEM((demand.shape[0] // 128, 128), jnp.int32),
            pltpu.VMEM((fac_n // 128, 128), F32),
            pltpu.VMEM((fac_n // 128, 128), F32),
            pltpu.VMEM((fac_n // 128, 128), F32),
            pltpu.VMEM((demand.shape[0] // 128, 128), F32),
            dma((8,)),
            pltpu.VMEM((nz, half, width), BF16),
            pltpu.VMEM((nz, half, 128), BF16),
            pltpu.VMEM((ng, width + 128, cols), BF16),
            pltpu.VMEM((nz, 8, 128), F32),
            pltpu.VMEM((ng, 8, cols), F32),
            pltpu.VMEM((ny, CORES * crows, 128), F32),
            pltpu.VMEM((tall * half, cols), F32),
            pltpu.VMEM((tall * half, cols), F32),
            pltpu.VMEM((nz, half, 128), F32),
            pltpu.VMEM((ng, 8, cols), F32),
            pltpu.VMEM((8, 128), F32),
            pltpu.VMEM((ng, 8, cols), F32),
            pltpu.VMEM((ny, CORES * crows, 128), F32),
            pltpu.VMEM((hrows * nz, 128), F32),
            pltpu.VMEM((hrows * nz, 128), F32),
            pltpu.VMEM((hrows * nz, 128), F32),
            pltpu.VMEM((8, 128), F32),
            pltpu.VMEM((ITERS * ny, ng, CORES * crows, 128), F32),
            pltpu.VMEM((ITERS * groups, nx, tall * hrows + 8, 128), F32),
            pltpu.VMEM((ITERS * groups, nz, tall * hrows + 8, 128), F32),
            pltpu.VMEM((nz, ny * crows, 128), F32),
            pltpu.VMEM((ng, 8, 128), F32),
            dma((nz,)), dma((nz,)), dma(()), dma(()), dma((ng,)), dma((ng,)), dma((ny,)),
            dma((ITERS * ny,)), dma((ITERS * ny,)), dma((ITERS * groups,)), dma((ITERS * groups,)),
            dma((ITERS * groups,)), dma((ITERS * groups,)), dma(()), dma(()), dma(()), dma(()),
        ],
        compiler_params=pltpu.CompilerParams(
            collective_id=0,
            has_side_effects=True,
            vmem_limit_bytes=60 * 1024 * 1024,
        ),
        name="dual",
    )(
        fac_coords, cust_coords, view(open_flags), view(demand), view(fixed_cost), view(capacity),
        view(cap_mult), view(cover_mult),
    )
    return lam.reshape(-1), mu.reshape(-1), bounds[:ITERS, 0]


def solution(mesh, dims=(4, 8, 4)):
    return jax.shard_map(
        functools.partial(local, dims),
        mesh=mesh,
        in_specs=(
            P("fac", None),
            P(("cust", "fac"), None),
            P("fac"),
            P("cust"),
            P("fac"),
            P("fac"),
            P("fac"),
            P("cust"),
        ),
        out_specs=(P("cust"), P("fac"), P()),
        check_vma=False,
    )
```
